32 devices in a mesh: col: 8 (over y, x, core), cuts: 4 (over z).
Axes of the slice: x: 2, y: 2, z: 4, core: 2. Of those that a mesh axis runs over, the one named last changes fastest.
Arguments:
- layout: int32 [16, 8], P(None, 'col'), may hold values from 0 to 15
- assign: int32 [16, 8], P('cuts', 'col'), may hold values from 0 to 3
- edge: bfloat16 [16, 64, 128], replicated, may hold values from -3 to 3
- gate_left: bfloat16 [8, 16, 64, 128], P('col'), may hold values from -1.5 to 1.5
- gate_right: bfloat16 [8, 16, 64, 128], P('col'), may hold values from -1.5 to 1.5
- phase_angle: float32 [4, 64], replicated, may hold values from -3.140625 to 3.140625
- close: float32 [16, 64, 128], replicated, may hold values from -6 to 6
Outputs:
- slice_amplitude: float32 [16, 2], P('cuts')
- slice_log: float32 [16], P('cuts')
- total_amp: float32 [2], replicated
- top_log: float32 [], replicated
The draws below stay inside these ranges and needn't reach their ends.
All inputs are finite; a program needn't handle non-finite values. Where the reference program divides by a largest or mean magnitude, that divisor is 1e-20 or more.
Results may differ from the reference program's by a relative error of at most 0.0003.
Values sent between devices are 32-bit elements; how exact they have to be, the bound alone decides.
A program may use at most 64 MiB of HBM per device.

```python
import math
import jax
import jax.numpy as jnp
from jax import lax

ROWS = 16
CHI = 64
NG = 16
QV = 4
COLS = 8
SLICES = 16


def plant(array, rng, low, top_value):
    index_at = [jax.random.randint(jax.random.fold_in(rng, axis), (), 0, length) for axis, length in enumerate(array.shape)]
    longest = array.shape.index(max(array.shape))
    neighbour = index_at[:longest] + [(index_at[longest] + 1) % array.shape[longest]] + index_at[longest + 1:]
    return array.at[tuple(index_at)].set(low).at[tuple(neighbour)].set(top_value)


def level_of(key, dims, shards, low, top_value):
    loudness, own = 1.0, jax.random.fold_in(key, 6)
    for axis_at, shards_of in shards:
        draws = jnp.exp(jax.random.uniform(jax.random.fold_in(own, axis_at), (shards_of,), jnp.float32, low / len(shards), top_value / len(shards)))
        loudness = loudness * jnp.repeat(draws, dims[axis_at] // shards_of).reshape([-1 if axis == axis_at else 1 for axis in range(len(dims))])
    return loudness


def scatter_about(rng, shape, scale, limit, pieces=(), dtype=jnp.bfloat16):
    entries = scale * jax.random.normal(rng, shape, jnp.float32)
    if pieces:
        entries = entries * level_of(rng, shape, pieces, -0.22, 0.18)
    return jnp.clip(entries, -limit, limit).astype(dtype)


def setup_inputs(seed: int = 0) -> dict:
    arg_keys = jax.random.split(jax.random.key(seed), 8)
    return {
        "layout": plant(jax.random.randint(arg_keys[0], (ROWS, COLS), 0, NG), jax.random.fold_in(arg_keys[0], 1), 0, NG - 1).astype(jnp.int32),
        "assign": plant(jax.random.randint(arg_keys[1], (SLICES, COLS), 0, QV), jax.random.fold_in(arg_keys[1], 1), 0, QV - 1).astype(jnp.int32),
        "edge": scatter_about(arg_keys[2], (ROWS, CHI, 2 * CHI), 0.5, 3.0),
        "gate_left": scatter_about(arg_keys[3], (COLS, NG, CHI, 2 * CHI), (CHI // 4) ** -0.5, 1.5, ((0, 8),)),
        "gate_right": scatter_about(arg_keys[4], (COLS, NG, CHI, 2 * CHI), (CHI // 4) ** -0.5, 1.5, ((0, 8),)),
        "phase_angle": jnp.clip(jax.random.uniform(arg_keys[5], (QV, CHI), jnp.float32, -3.140625, 3.140625), -3.140625, 3.140625),
        "close": scatter_about(arg_keys[6], (ROWS, CHI, 2 * CHI), 1.0, 6.0, (), jnp.float32),
    }


def sweep_column(board, scales, left_sel, right_sel, cosine, sine):
    width = board.shape[-2]
    below = jnp.concatenate([board[:, 1:], jnp.zeros_like(board[:, :1])], axis=1)
    mixed = board + 0.5 * below
    left_four = left_sel.astype(jnp.float32).reshape(left_sel.shape[0], width, 2, width)
    stacked = jnp.einsum('rpka,srab->srkpb', left_four, mixed, precision=lax.Precision.HIGHEST)
    former = stacked[:, :, 0]
    latter = stacked[:, :, 1]
    real_part = former[..., :width] - latter[..., width:]
    imag_part = former[..., width:] + latter[..., :width]
    right_wide = right_sel.astype(jnp.float32)
    from_real = jnp.einsum('srab,rbq->sraq', real_part, right_wide, precision=lax.Precision.HIGHEST)
    from_imag = jnp.einsum('srab,rbq->sraq', imag_part, right_wide, precision=lax.Precision.HIGHEST)
    out_real = from_real[..., :width] - from_imag[..., width:]
    out_imag = from_real[..., width:] + from_imag[..., :width]
    cos_rows = cosine[:, None, None, :]
    sin_rows = sine[:, None, None, :]
    turned_real = out_real * cos_rows - out_imag * sin_rows
    turned_imag = out_real * sin_rows + out_imag * cos_rows
    peaks = jnp.maximum(lax.optimization_barrier(jnp.max(jnp.abs(turned_real), axis=(1, 2, 3))), lax.optimization_barrier(jnp.max(jnp.abs(turned_imag), axis=(1, 2, 3))))
    peaks = jnp.maximum(peaks, 1.0)
    board = jnp.concatenate([turned_real, turned_imag], -1) / peaks[:, None, None, None]
    return (board, scales + jnp.log(peaks))

def amplitude(board, close):
    width = close.shape[-1] // 2
    b_real = board[..., :width]
    b_imag = board[..., width:]
    c_real = close[..., :width]
    c_imag = close[..., width:]
    factor = 1.0 / math.sqrt(close.shape[0] * width * width)
    amp_real = lax.optimization_barrier(jnp.sum(b_real * c_real - b_imag * c_imag, axis=(1, 2, 3))) * factor
    amp_imag = lax.optimization_barrier(jnp.sum(b_real * c_imag + b_imag * c_real, axis=(1, 2, 3))) * factor
    return jnp.stack([amp_real, amp_imag], -1)

def reference(layout, assign, edge, gate_left, gate_right, phase_angle, close):
    count = assign.shape[0]
    board = jnp.broadcast_to(edge.astype(jnp.float32)[None], (count,) + edge.shape)
    scales = jnp.zeros((count,), jnp.float32)
    cos_table = jnp.cos(phase_angle)
    sin_table = jnp.sin(phase_angle)

    def advance(carry, inputs):
        board, scales = carry
        left_col, right_col, kinds, values = inputs
        left_sel = left_col[kinds.astype(jnp.int32)]
        right_sel = right_col[kinds.astype(jnp.int32)]
        cosine = cos_table[values.astype(jnp.int32)]
        sine = sin_table[values.astype(jnp.int32)]
        return (sweep_column(board, scales, left_sel, right_sel, cosine, sine), None)
    (board, scales), unused = lax.scan(advance, (board, scales), (gate_left, gate_right, layout.T, assign.T))
    amps = amplitude(board, close)
    top_log = jnp.max(scales)
    total_amp = lax.optimization_barrier(jnp.sum(amps * jnp.exp(scales - top_log)[:, None], axis=0))
    return (amps, scales, total_amp, top_log)
```

```python
import functools
import math

import jax
import jax.numpy as jnp
from jax import lax
from jax.experimental import pallas as pl
from jax.experimental.pallas import tpu as pltpu
from jax.sharding import PartitionSpec as P

MESH = pl.DeviceIdType.MESH
SEGMENT = 8


def split(value):
    high = value.astype(jnp.bfloat16)
    low = (value - high.astype(jnp.float32)).astype(jnp.bfloat16)
    return high, low


def swap(value, width):
    return pltpu.roll(value, width, len(value.shape) - 1)


def kernel(
    n, nz, rows,
    layout_ref, assign_ref, edge_ref, left_ref, right_ref, cos_ref, sin_ref, close_ref,
    amp_ref, log_ref, total_ref, top_ref,
    stage, stage_phase, gates, phases, board, halo, peak, xsend, xrecv, zsend, zrecv,
    gate_send, gate_recv, halo_send, halo_recv, x_send, x_recv, z_send, z_recv,
):
    me = lax.axis_index("col")
    mz = lax.axis_index("cuts")
    per_col = left_ref.shape[0]
    columns = n * per_col
    own = rows // n
    slices = assign_ref.shape[0]
    width = left_ref.shape[2]
    lanes = 2 * width
    last = me == n - 1

    barrier = pltpu.get_barrier_semaphore()
    for k in range(1, n):
        pl.semaphore_signal(
            barrier, inc=1, device_id=(lax.rem(me + k, n), mz), device_id_type=MESH
        )
    for k in range(1, nz):
        pl.semaphore_signal(
            barrier, inc=1, device_id=(me, lax.rem(mz + k, nz)), device_id_type=MESH
        )

    lane = lax.broadcasted_iota(jnp.int32, (1, lanes), 1)
    sign = jnp.where(lane < width, -1.0, 1.0).astype(jnp.float32)

    for cl in range(per_col):
        for s in range(slices):
            value = assign_ref[s, cl]
            stage_phase[cl, pl.ds(s, 1), :] = cos_ref[pl.ds(value, 1), :]
            stage_phase[cl, pl.ds(slices + s, 1), :] = sin_ref[pl.ds(value, 1), :] * sign
        for r in range(rows):
            kind = layout_ref[r, cl]
            stage[cl, 0, r] = left_ref[cl, kind].astype(jnp.float32)
            stage[cl, 1, r] = right_ref[cl, kind].astype(jnp.float32)
    for s in range(slices):
        peak[s] = jnp.ones(peak.shape[1:], jnp.float32)

    @pl.when(last)
    def _():
        halo[...] = jnp.zeros_like(halo)

    def gate_copy(cl, part, target):
        column = me * per_col + cl
        if part == 2:
            source, sink = stage_phase.at[cl], phases.at[column]
        else:
            source = stage.at[cl, part, pl.ds(target * own, own)]
            sink = gates.at[column, part]
        return pltpu.make_async_remote_copy(
            src_ref=source,
            dst_ref=sink,
            send_sem=gate_send.at[cl, part, target],
            recv_sem=gate_recv.at[column, part],
            device_id=(target, mz),
            device_id_type=MESH,
        )

    pl.semaphore_wait(barrier, n - 1 + nz - 1)
    for cl in range(per_col):
        for part in (2, 0, 1):
            for k in range(1, n):
                gate_copy(cl, part, lax.rem(me + k, n)).start()
    for cl in range(per_col):
        column = me * per_col + cl
        phases[column] = stage_phase[cl]
        for part in range(2):
            gates[column, part] = stage[cl, part, pl.ds(me * own, own)]

    def wait_gates(column, part):
        sink = phases.at[column] if part == 2 else gates.at[column, part]

        @pl.when(column // per_col != me)
        def _():
            pltpu.make_async_remote_copy(
                src_ref=sink,
                dst_ref=sink,
                send_sem=gate_send.at[0, part, 0],
                recv_sem=gate_recv.at[column, part],
                device_id=(lax.rem(me + 1, n), mz),
                device_id_type=MESH,
            ).wait_recv()

    def halo_copy(column):
        return pltpu.make_async_remote_copy(
            src_ref=board.at[column, 0],
            dst_ref=halo.at[column],
            send_sem=halo_send.at[column],
            recv_sem=halo_recv.at[column],
            device_id=(lax.rem(me + n - 1, n), mz),
            device_id_type=MESH,
        )

    def one_row(column, r, mixed, right_wait):
        left = gates[column, 0, r].astype(jnp.bfloat16)
        left = jnp.concatenate([left, left], axis=1)
        stacks = []
        for m in mixed:
            high, low = split(m)
            turned_high, turned_low = split(swap(m, width) * sign)
            stacks.append(jnp.concatenate([high, turned_high, low, turned_low], axis=0))
        middle = jnp.dot(
            left, jnp.concatenate(stacks, axis=1), preferred_element_type=jnp.float32
        )
        if right_wait:
            wait_gates(column, 1)
            wait_gates(column, 2)
        right = gates[column, 1, r]
        right = jnp.concatenate([right, swap(right, width) * sign], axis=0).astype(jnp.bfloat16)
        right = jnp.concatenate([right, right], axis=0)
        high, low = split(
            jnp.concatenate([middle[:, i * lanes:(i + 1) * lanes] for i in range(len(mixed))], axis=0)
        )
        outs = jnp.dot(
            jnp.concatenate([high, low], axis=1), right, preferred_element_type=jnp.float32
        )
        for s in range(slices):
            i = s if len(mixed) > 1 else 0
            out = outs[i * width:(i + 1) * width]
            if len(mixed) == 1 and s > 0:
                out_swapped = first_swapped
            else:
                out_swapped = swap(out, width)
                first_swapped = out_swapped
            turned = out * phases[column, pl.ds(s, 1), :] + out_swapped * phases[
                column, pl.ds(slices + s, 1), :
            ]
            board[column, r, s] = turned
            size = jnp.abs(turned).reshape(width // 8, 8, lanes)
            peak[s] = jnp.maximum(peak[s], jnp.max(size, axis=0))

    def after_row(column, r):
        if r == 0:
            @pl.when(me > 0)
            def _():
                halo_copy(column).start()

    wait_gates(0, 0)
    for r in range(own):
        row = me * own + r
        here = edge_ref[row].astype(jnp.float32)
        if r + 1 < own:
            below = 0.5 * edge_ref[row + 1].astype(jnp.float32)
        else:
            weight = jnp.where(last, 0.0, 0.5).astype(jnp.float32)
            below = weight * edge_ref[jnp.minimum(row + 1, rows - 1)].astype(jnp.float32)
        one_row(0, r, [here + below], r == 0)
        if columns > 1:
            after_row(0, r)

    def column_step(column, scale, send):
        wait_gates(column, 0)
        for r in range(own):
            if r + 1 == own:
                @pl.when(jnp.logical_not(last))
                def _():
                    halo_copy(column - 1).wait_recv()
            mixed = []
            for s in range(slices):
                below = board[column - 1, r + 1, s] if r + 1 < own else halo[column - 1, s]
                m = board[column - 1, r, s] + 0.5 * below
                mixed.append(m if scale is None else m * scale[s])
            one_row(column, r, mixed, r == 0)
            if send:
                after_row(column, r)

    def exchange(slot, count, index, axis_copy, sender, receiver):
        def copy(target):
            return axis_copy(slot, target)

        receiver[slot, index] = sender[slot]
        for k in range(1, count):
            copy(lax.rem(index + k, count)).start()
        for k in range(1, count):
            copy(lax.rem(index + k, count)).wait_send()

    def x_copy(slot, target):
        return pltpu.make_async_remote_copy(
            src_ref=xsend.at[slot],
            dst_ref=xrecv.at[slot, me],
            send_sem=x_send.at[slot, target],
            recv_sem=x_recv.at[slot, me],
            device_id=(target, mz),
            device_id_type=MESH,
        )

    def x_wait(slot):
        for k in range(1, n):
            source = lax.rem(me + k, n)
            pltpu.make_async_remote_copy(
                src_ref=xsend.at[slot],
                dst_ref=xrecv.at[slot, source],
                send_sem=x_send.at[slot, source],
                recv_sem=x_recv.at[slot, source],
                device_id=(source, mz),
                device_id_type=MESH,
            ).wait_recv()

    def z_copy(target):
        return pltpu.make_async_remote_copy(
            src_ref=zsend,
            dst_ref=zrecv.at[mz],
            send_sem=z_send.at[target],
            recv_sem=z_recv.at[mz],
            device_id=(me, target),
            device_id_type=MESH,
        )

    def local_peaks():
        return [
            jnp.max(jnp.max(peak[s], axis=0, keepdims=True), axis=1, keepdims=True)
            for s in range(slices)
        ]

    logs = [jnp.zeros((1, 1), jnp.float32)] * slices
    scale = None
    begin, slot = 1, 0
    while True:
        stop = min(columns, (begin // SEGMENT + 1) * SEGMENT)
        if scale is not None:
            column_step(begin, scale, begin + 1 < columns)
            begin += 1
        full = min(stop, columns - 1)

        def loop_step(column, carry):
            column_step(column, None, True)
            return carry

        if full > begin:
            lax.fori_loop(begin, full, loop_step, 0)
        if stop == columns:
            if columns - 1 >= begin:
                column_step(columns - 1, None, False)
            break
        for s, m in enumerate(local_peaks()):
            xsend[slot, pl.ds(s, 1), :] = jnp.broadcast_to(m, (1, lanes))
        exchange(slot, n, me, x_copy, xsend, xrecv)
        x_wait(slot)
        scale = []
        for s in range(slices):
            m = xrecv[slot, 0, pl.ds(s, 1), :]
            for d in range(1, n):
                m = jnp.maximum(m, xrecv[slot, d, pl.ds(s, 1), :])
            logs[s] = logs[s] + jnp.log(m[:, :1])
            scale.append(1.0 / m)
            peak[s] = jnp.ones(peak.shape[1:], jnp.float32)
        begin, slot = stop, slot + 1

    factor = 1.0 / math.sqrt(rows * width * width)
    mine = local_peaks()
    for s in range(slices):
        real = jnp.zeros((8, lanes), jnp.float32)
        imag = jnp.zeros((8, lanes), jnp.float32)
        inverse = 1.0 / mine[s]
        for r in range(own):
            close = close_ref[me * own + r]
            value = board[columns - 1, r, s] * inverse
            real = real + jnp.sum((value * close).reshape(width // 8, 8, lanes), axis=0)
            imag = imag + jnp.sum((value * swap(close, width)).reshape(width // 8, 8, lanes), axis=0)
        xsend[slot, pl.ds(s, 1), :] = jnp.sum(real, axis=0, keepdims=True) * (-sign)
        xsend[slot, pl.ds(slices + s, 1), :] = jnp.sum(imag, axis=0, keepdims=True)
        xsend[slot, pl.ds(2 * slices + s, 1), :] = jnp.broadcast_to(mine[s], (1, lanes))
    exchange(slot, n, me, x_copy, xsend, xrecv)
    x_wait(slot)
    all_peaks = [xrecv[slot, d, pl.ds(2 * slices, slices), :] for d in range(n)]
    top_peak = functools.reduce(jnp.maximum, all_peaks)
    inverse = 1.0 / top_peak
    real = jnp.zeros((slices, lanes), jnp.float32)
    imag = jnp.zeros((slices, lanes), jnp.float32)
    for d in range(n):
        ratio = all_peaks[d] * inverse
        real = real + xrecv[slot, d, pl.ds(0, slices), :] * ratio
        imag = imag + xrecv[slot, d, pl.ds(slices, slices), :] * ratio
    real = jnp.sum(real, axis=1, keepdims=True) * factor
    imag = jnp.sum(imag, axis=1, keepdims=True) * factor
    log = jnp.log(top_peak)[:, :1] + jnp.concatenate(logs, axis=0)
    amp_ref[...] = jnp.concatenate([real, imag], axis=1)
    log_ref[...] = log
    top = jnp.max(log, axis=0, keepdims=True)
    share = jnp.exp(log - top)
    zsend[pl.ds(0, 1), :] = jnp.broadcast_to(jnp.sum(real * share, axis=0, keepdims=True), (1, lanes))
    zsend[pl.ds(1, 1), :] = jnp.broadcast_to(jnp.sum(imag * share, axis=0, keepdims=True), (1, lanes))
    zsend[pl.ds(2, 1), :] = jnp.broadcast_to(top, (1, lanes))
    zrecv[mz] = zsend[...]
    for k in range(1, nz):
        z_copy(lax.rem(mz + k, nz)).start()
    for k in range(1, nz):
        source = lax.rem(mz + k, nz)
        pltpu.make_async_remote_copy(
            src_ref=zsend,
            dst_ref=zrecv.at[source],
            send_sem=z_send.at[source],
            recv_sem=z_recv.at[source],
            device_id=(me, source),
            device_id_type=MESH,
        ).wait_recv()
    tops = [zrecv[z, pl.ds(2, 1), :] for z in range(nz)]
    top = functools.reduce(jnp.maximum, tops)
    real = jnp.zeros((1, lanes), jnp.float32)
    imag = jnp.zeros((1, lanes), jnp.float32)
    for z in range(nz):
        share = jnp.exp(tops[z] - top)
        real = real + zrecv[z, pl.ds(0, 1), :] * share
        imag = imag + zrecv[z, pl.ds(1, 1), :] * share
    total_ref[...] = jnp.concatenate([real[:, :1], imag[:, :1]], axis=1)
    top_ref[...] = top[:, :1]

    for k in range(1, nz):
        z_copy(lax.rem(mz + k, nz)).wait_send()
    for cl in range(per_col):
        for part in range(3):
            for k in range(1, n):
                gate_copy(cl, part, lax.rem(me + k, n)).wait_send()
    if columns > 1:
        @pl.when(me > 0)
        def _():
            for column in range(columns - 1):
                halo_copy(column).wait_send()


def body(layout, assign, edge, gate_left, gate_right, phase_angle, close):
    n, nz = lax.axis_size("col"), lax.axis_size("cuts")
    rows, width, lanes = edge.shape
    per_col = gate_left.shape[0]
    columns, own, slices = n * per_col, rows // n, assign.shape[0]
    rounds = -(-columns // SEGMENT)
    cosine, sine = jnp.cos(phase_angle), jnp.sin(phase_angle)
    cosine = jnp.concatenate([cosine, cosine], axis=1)
    sine = jnp.concatenate([sine, sine], axis=1)
    f32 = jnp.float32
    vmem = pl.BlockSpec(memory_space=pltpu.VMEM)
    smem = pl.BlockSpec(memory_space=pltpu.SMEM)
    dma = pltpu.SemaphoreType.DMA
    message = -(-3 * slices // 8) * 8
    phase_rows = -(-2 * slices // 8) * 8
    amp, log, total, top = pl.pallas_call(
        functools.partial(kernel, n, nz, rows),
        out_shape=[
            jax.ShapeDtypeStruct((slices, 2), f32),
            jax.ShapeDtypeStruct((slices, 1), f32),
            jax.ShapeDtypeStruct((1, 2), f32),
            jax.ShapeDtypeStruct((1, 1), f32),
        ],
        in_specs=[smem, smem] + [vmem] * 6,
        out_specs=[vmem] * 4,
        scratch_shapes=[
            pltpu.VMEM((per_col, 2, rows, width, lanes), f32),
            pltpu.VMEM((per_col, phase_rows, lanes), f32),
            pltpu.VMEM((columns, 2, own, width, lanes), f32),
            pltpu.VMEM((columns, phase_rows, lanes), f32),
            pltpu.VMEM((columns, own, slices, width, lanes), f32),
            pltpu.VMEM((columns, slices, width, lanes), f32),
            pltpu.VMEM((slices, 8, lanes), f32),
            pltpu.VMEM((rounds, message, lanes), f32),
            pltpu.VMEM((rounds, n, message, lanes), f32),
            pltpu.VMEM((8, lanes), f32),
            pltpu.VMEM((nz, 8, lanes), f32),
            dma((per_col, 3, n)),
            dma((columns, 3)),
            dma((columns,)),
            dma((columns,)),
            dma((rounds, n)),
            dma((rounds, n)),
            dma((nz,)),
            dma((nz,)),
        ],
        compiler_params=pltpu.CompilerParams(
            collective_id=0, has_side_effects=True, vmem_limit_bytes=48 * 1024 * 1024
        ),
    )(layout, assign, edge, gate_left, gate_right, cosine, sine, close)
    return amp, log.reshape(slices), total.reshape(2), top.reshape(())


def solution(mesh):
    in_specs = (
        P(None, "col"),
        P("cuts", "col"),
        P(),
        P("col", None, None, None),
        P("col", None, None, None),
        P(),
        P(),
    )
    out_specs = (P("cuts", None), P("cuts"), P(), P())
    return jax.shard_map(body, mesh=mesh, in_specs=in_specs, out_specs=out_specs, check_vma=False)
```

```python
import functools
import math

import jax
import jax.numpy as jnp
from jax import lax
from jax.experimental import pallas as pl
from jax.experimental.pallas import tpu as pltpu
from jax.sharding import PartitionSpec as P

MESH = pl.DeviceIdType.MESH
SEGMENT = 8


def split(value):
    high = value.astype(jnp.bfloat16)
    low = (value - high.astype(jnp.float32)).astype(jnp.bfloat16)
    return high, low


def swap(value, width):
    return pltpu.roll(value, width, len(value.shape) - 1)


def position(device, n):
    if n % 8:
        return device
    chip = lax.rem(device // 2, 4)
    return device + 2 * (chip // 2) * (1 - 2 * lax.rem(chip, 2))


device_at = position


def kernel(
    n, nz, rows,
    layout_ref, assign_ref, edge_hbm, left_hbm, right_hbm, angle_ref, close_hbm,
    amp_ref, log_ref, total_ref, top_ref,
    edge_ref, left_ref, right_ref, close_ref, cos_ref, sin_ref, load_sem, stage, stage_phase, gates, phases, board, halo, peak, xsend, xrecv, zsend, zrecv,
    gate_send, gate_recv, halo_send, halo_recv, x_send, x_recv, z_send, z_recv,
):
    me = lax.axis_index("col")
    mz = lax.axis_index("cuts")
    per_col = left_ref.shape[0]
    columns = n * per_col
    own = rows // n
    slices = assign_ref.shape[1]
    pieces = 2 if slices % 2 == 0 else 1
    part_size = slices // pieces
    width = left_ref.shape[2]
    lanes = 2 * width
    place = position(me, n)
    last = place == n - 1
    next_row = jnp.minimum((place + 1) * own, rows - 1)
    loads = [
        pltpu.make_async_copy(left_hbm, left_ref, load_sem.at[0]),
        pltpu.make_async_copy(right_hbm, right_ref, load_sem.at[1]),
        pltpu.make_async_copy(
            edge_hbm.at[pl.ds(place * own, own)], edge_ref.at[pl.ds(0, own)], load_sem.at[2]
        ),
        pltpu.make_async_copy(
            edge_hbm.at[pl.ds(next_row, 1)], edge_ref.at[pl.ds(own, 1)], load_sem.at[3]
        ),
        pltpu.make_async_copy(close_hbm.at[pl.ds(place * own, own)], close_ref, load_sem.at[4]),
    ]
    for load in loads:
        load.start()

    barrier = pltpu.get_barrier_semaphore()
    for k in range(1, n):
        pl.semaphore_signal(
            barrier, inc=1, device_id=(lax.rem(me + k, n), mz), device_id_type=MESH
        )
    for k in range(1, nz):
        pl.semaphore_signal(
            barrier, inc=1, device_id=(me, lax.rem(mz + k, nz)), device_id_type=MESH
        )

    lane = lax.broadcasted_iota(jnp.int32, (1, lanes), 1)
    sign = jnp.where(lane < width, -1.0, 1.0).astype(jnp.float32)

    angle = angle_ref[...]
    cosine, sine = jnp.cos(angle), jnp.sin(angle)
    cos_ref[...] = jnp.concatenate([cosine, cosine], axis=1)
    sin_ref[...] = jnp.concatenate([-sine, sine], axis=1)
    for s in range(slices):
        peak[s] = jnp.ones(peak.shape[1:], jnp.float32)

    @pl.when(last)
    def _():
        halo[...] = jnp.zeros_like(halo)

    loads[0].wait()
    loads[1].wait()
    for cl in range(per_col):
        for s in range(slices):
            value = assign_ref[cl, s]
            stage_phase[cl, pl.ds(s, 1), :] = cos_ref[pl.ds(value, 1), :]
            stage_phase[cl, pl.ds(slices + s, 1), :] = sin_ref[pl.ds(value, 1), :]
        for r in range(rows):
            kind = layout_ref[cl, r]
            stage[cl, 0, r] = left_ref[cl, kind].astype(jnp.float32)
            stage[cl, 1, r] = right_ref[cl, kind].astype(jnp.float32)

    def gate_copy(cl, part, target):
        column = me * per_col + cl
        if part == 2:
            source, sink = stage_phase.at[cl], phases.at[column]
        else:
            source = stage.at[cl, part, pl.ds(position(target, n) * own, own)]
            sink = gates.at[column, part]
        return pltpu.make_async_remote_copy(
            src_ref=source,
            dst_ref=sink,
            send_sem=gate_send.at[cl, part, target],
            recv_sem=gate_recv.at[column, part],
            device_id=(target, mz),
            device_id_type=MESH,
        )

    pl.semaphore_wait(barrier, n - 1 + nz - 1)
    for cl in range(per_col):
        for k in range(1, n):
            target = device_at(lax.rem(place + n - k, n), n)
            for part in (2, 0, 1):
                gate_copy(cl, part, target).start()
    for cl in range(per_col):
        column = me * per_col + cl
        phases[column] = stage_phase[cl]
        for part in range(2):
            gates[column, part] = stage[cl, part, pl.ds(place * own, own)]

    def wait_gates(column, part):
        sink = phases.at[column] if part == 2 else gates.at[column, part]

        @pl.when(column // per_col != me)
        def _():
            pltpu.make_async_remote_copy(
                src_ref=sink,
                dst_ref=sink,
                send_sem=gate_send.at[0, part, 0],
                recv_sem=gate_recv.at[column, part],
                device_id=(lax.rem(me + 1, n), mz),
                device_id_type=MESH,
            ).wait_recv()

    def halo_copy(column, piece):
        part = pl.ds(piece * part_size, part_size)
        return pltpu.make_async_remote_copy(
            src_ref=board.at[column, 0, part],
            dst_ref=halo.at[column, part],
            send_sem=halo_send.at[column, piece],
            recv_sem=halo_recv.at[column, piece],
            device_id=(device_at(lax.rem(place + n - 1, n), n), mz),
            device_id_type=MESH,
        )

    def one_row(column, r, mixed, right_wait, send):
        left = gates[column, 0, r].astype(jnp.bfloat16)
        left = jnp.concatenate([left, left], axis=1)
        stacks = []
        for m in mixed:
            high, low = split(m)
            turned_high, turned_low = split(swap(m, width) * sign)
            stacks.append(jnp.concatenate([high, turned_high, low, turned_low], axis=0))
        middle = jnp.dot(
            left, jnp.concatenate(stacks, axis=1), preferred_element_type=jnp.float32
        )
        if right_wait:
            wait_gates(column, 1)
            wait_gates(column, 2)
        right = gates[column, 1, r]
        right = jnp.concatenate([right, swap(right, width) * sign], axis=0).astype(jnp.bfloat16)
        right = jnp.concatenate([right, right], axis=0)
        high, low = split(
            jnp.concatenate([middle[:, i * lanes:(i + 1) * lanes] for i in range(len(mixed))], axis=0)
        )
        outs = jnp.dot(
            jnp.concatenate([high, low], axis=1), right, preferred_element_type=jnp.float32
        )
        for s in range(slices):
            i = s if len(mixed) > 1 else 0
            out = outs[i * width:(i + 1) * width]
            if len(mixed) == 1 and s > 0:
                out_swapped = first_swapped
            else:
                out_swapped = swap(out, width)
                first_swapped = out_swapped
            turned = out * phases[column, pl.ds(s, 1), :] + out_swapped * phases[
                column, pl.ds(slices + s, 1), :
            ]
            board[column, r, s] = turned
            size = jnp.abs(turned).reshape(width // 8, 8, lanes)
            peak[s] = jnp.maximum(peak[s], jnp.max(size, axis=0))
            if send and (s + 1) % part_size == 0:
                @pl.when(place > 0)
                def _():
                    halo_copy(column, s // part_size).start()

    for load in loads[2:]:
        load.wait()
    wait_gates(0, 0)
    for r in range(own):
        below = edge_ref[r + 1].astype(jnp.float32)
        weight = 0.5 if r + 1 < own else jnp.where(last, 0.0, 0.5).astype(jnp.float32)
        mixed = edge_ref[r].astype(jnp.float32) + weight * below
        one_row(0, r, [mixed], r == 0, r == 0 and columns > 1)

    def column_step(column, scale, send):
        wait_gates(column, 0)
        for r in range(own):
            mixed = []
            for s in range(slices):
                if r + 1 == own and s % part_size == 0:
                    @pl.when(jnp.logical_not(last))
                    def _():
                        halo_copy(column - 1, s // part_size).wait_recv()
                below = board[column - 1, r + 1, s] if r + 1 < own else halo[column - 1, s]
                m = board[column - 1, r, s] + 0.5 * below
                mixed.append(m if scale is None else m * scale[s])
            one_row(column, r, mixed, r == 0, send and r == 0)

    def exchange(slot, count, index, axis_copy, sender, receiver):
        def copy(target):
            return axis_copy(slot, target)

        receiver[slot, index] = sender[slot]
        for k in range(1, count):
            copy(lax.rem(index + k, count)).start()
        for k in range(1, count):
            copy(lax.rem(index + k, count)).wait_send()

    def x_copy(slot, target):
        return pltpu.make_async_remote_copy(
            src_ref=xsend.at[slot],
            dst_ref=xrecv.at[slot, me],
            send_sem=x_send.at[slot, target],
            recv_sem=x_recv.at[slot, me],
            device_id=(target, mz),
            device_id_type=MESH,
        )

    def x_wait(slot):
        for k in range(1, n):
            source = lax.rem(me + k, n)
            pltpu.make_async_remote_copy(
                src_ref=xsend.at[slot],
                dst_ref=xrecv.at[slot, source],
                send_sem=x_send.at[slot, source],
                recv_sem=x_recv.at[slot, source],
                device_id=(source, mz),
                device_id_type=MESH,
            ).wait_recv()

    def z_copy(target):
        return pltpu.make_async_remote_copy(
            src_ref=zsend,
            dst_ref=zrecv.at[mz],
            send_sem=z_send.at[target],
            recv_sem=z_recv.at[mz],
            device_id=(me, target),
            device_id_type=MESH,
        )

    def local_peaks():
        return [
            jnp.max(jnp.max(peak[s], axis=0, keepdims=True), axis=1, keepdims=True)
            for s in range(slices)
        ]

    logs = [jnp.zeros((1, 1), jnp.float32)] * slices
    scale = None
    begin, slot = 1, 0
    while True:
        stop = min(columns, (begin // SEGMENT + 1) * SEGMENT)
        if scale is not None:
            column_step(begin, scale, begin + 1 < columns)
            begin += 1
        full = min(stop, columns - 1)

        def loop_step(column, carry):
            column_step(column, None, True)
            return carry

        if full > begin:
            lax.fori_loop(begin, full, loop_step, 0)
        if stop == columns:
            if columns - 1 >= begin:
                column_step(columns - 1, None, False)
            break
        for s, m in enumerate(local_peaks()):
            xsend[slot, pl.ds(s, 1), :] = jnp.broadcast_to(m, (1, lanes))
        exchange(slot, n, me, x_copy, xsend, xrecv)
        x_wait(slot)
        scale = []
        for s in range(slices):
            m = xrecv[slot, 0, pl.ds(s, 1), :]
            for d in range(1, n):
                m = jnp.maximum(m, xrecv[slot, d, pl.ds(s, 1), :])
            logs[s] = logs[s] + jnp.log(m[:, :1])
            scale.append(1.0 / m)
            peak[s] = jnp.ones(peak.shape[1:], jnp.float32)
        begin, slot = stop, slot + 1

    factor = 1.0 / math.sqrt(rows * width * width)
    mine = local_peaks()
    for s in range(slices):
        real = jnp.zeros((8, lanes), jnp.float32)
        imag = jnp.zeros((8, lanes), jnp.float32)
        inverse = 1.0 / mine[s]
        for r in range(own):
            close = close_ref[r]
            value = board[columns - 1, r, s] * inverse
            real = real + jnp.sum((value * close).reshape(width // 8, 8, lanes), axis=0)
            imag = imag + jnp.sum((value * swap(close, width)).reshape(width // 8, 8, lanes), axis=0)
        xsend[slot, pl.ds(s, 1), :] = jnp.sum(real, axis=0, keepdims=True) * (-sign)
        xsend[slot, pl.ds(slices + s, 1), :] = jnp.sum(imag, axis=0, keepdims=True)
        xsend[slot, pl.ds(2 * slices + s, 1), :] = jnp.broadcast_to(mine[s], (1, lanes))
    exchange(slot, n, me, x_copy, xsend, xrecv)
    x_wait(slot)
    all_peaks = [xrecv[slot, d, pl.ds(2 * slices, slices), :] for d in range(n)]
    top_peak = functools.reduce(jnp.maximum, all_peaks)
    inverse = 1.0 / top_peak
    real = jnp.zeros((slices, lanes), jnp.float32)
    imag = jnp.zeros((slices, lanes), jnp.float32)
    for d in range(n):
        ratio = all_peaks[d] * inverse
        real = real + xrecv[slot, d, pl.ds(0, slices), :] * ratio
        imag = imag + xrecv[slot, d, pl.ds(slices, slices), :] * ratio
    real = jnp.sum(real, axis=1, keepdims=True) * factor
    imag = jnp.sum(imag, axis=1, keepdims=True) * factor
    log = jnp.log(top_peak)[:, :1] + jnp.concatenate(logs, axis=0)
    for s in range(slices):
        amp_ref[:, pl.ds(s, 1)] = jnp.concatenate([real[s:s + 1], imag[s:s + 1]], axis=0)
        log_ref[:, pl.ds(s, 1)] = log[s:s + 1]
    top = jnp.max(log, axis=0, keepdims=True)
    share = jnp.exp(log - top)
    zsend[pl.ds(0, 1), :] = jnp.broadcast_to(jnp.sum(real * share, axis=0, keepdims=True), (1, lanes))
    zsend[pl.ds(1, 1), :] = jnp.broadcast_to(jnp.sum(imag * share, axis=0, keepdims=True), (1, lanes))
    zsend[pl.ds(2, 1), :] = jnp.broadcast_to(top, (1, lanes))
    zrecv[mz] = zsend[...]
    for k in range(1, nz):
        z_copy(lax.rem(mz + k, nz)).start()
    for k in range(1, nz):
        source = lax.rem(mz + k, nz)
        pltpu.make_async_remote_copy(
            src_ref=zsend,
            dst_ref=zrecv.at[source],
            send_sem=z_send.at[source],
            recv_sem=z_recv.at[source],
            device_id=(me, source),
            device_id_type=MESH,
        ).wait_recv()
    tops = [zrecv[z, pl.ds(2, 1), :] for z in range(nz)]
    top = functools.reduce(jnp.maximum, tops)
    real = jnp.zeros((1, lanes), jnp.float32)
    imag = jnp.zeros((1, lanes), jnp.float32)
    for z in range(nz):
        share = jnp.exp(tops[z] - top)
        real = real + zrecv[z, pl.ds(0, 1), :] * share
        imag = imag + zrecv[z, pl.ds(1, 1), :] * share
    total_ref[...] = jnp.concatenate([real[:, :1], imag[:, :1]], axis=1)
    top_ref[...] = top[:, :1]

    for k in range(1, nz):
        z_copy(lax.rem(mz + k, nz)).wait_send()
    for cl in range(per_col):
        for part in range(3):
            for k in range(1, n):
                gate_copy(cl, part, lax.rem(me + k, n)).wait_send()
    if columns > 1:
        @pl.when(place > 0)
        def _():
            for column in range(columns - 1):
                for piece in range(pieces):
                    halo_copy(column, piece).wait_send()


def body(layout, assign, edge, gate_left, gate_right, phase_angle, close):
    n, nz = lax.axis_size("col"), lax.axis_size("cuts")
    rows, width, lanes = edge.shape
    per_col = gate_left.shape[0]
    columns, own, slices = n * per_col, rows // n, assign.shape[0]
    rounds = -(-columns // SEGMENT)
    pieces = 2 if slices % 2 == 0 else 1
    f32 = jnp.float32
    vmem = pl.BlockSpec(memory_space=pltpu.VMEM)
    hbm = pl.BlockSpec(memory_space=pltpu.HBM)
    smem = pl.BlockSpec(memory_space=pltpu.SMEM)
    dma = pltpu.SemaphoreType.DMA
    message = -(-3 * slices // 8) * 8
    phase_rows = -(-2 * slices // 8) * 8
    amp, log, total, top = pl.pallas_call(
        functools.partial(kernel, n, nz, rows),
        out_shape=[
            jax.ShapeDtypeStruct((2, slices), f32),
            jax.ShapeDtypeStruct((1, slices), f32),
            jax.ShapeDtypeStruct((1, 2), f32),
            jax.ShapeDtypeStruct((1, 1), f32),
        ],
        in_specs=[smem, smem, hbm, hbm, hbm, vmem, hbm],
        out_specs=[vmem] * 4,
        scratch_shapes=[
            pltpu.VMEM((own + 1, width, lanes), edge.dtype),
            pltpu.VMEM(gate_left.shape, gate_left.dtype),
            pltpu.VMEM(gate_right.shape, gate_right.dtype),
            pltpu.VMEM((own, width, lanes), f32),
            pltpu.VMEM((phase_angle.shape[0], lanes), f32),
            pltpu.VMEM((phase_angle.shape[0], lanes), f32),
            dma((5,)),
            pltpu.VMEM((per_col, 2, rows, width, lanes), f32),
            pltpu.VMEM((per_col, phase_rows, lanes), f32),
            pltpu.VMEM((columns, 2, own, width, lanes), f32),
            pltpu.VMEM((columns, phase_rows, lanes), f32),
            pltpu.VMEM((columns, own, slices, width, lanes), f32),
            pltpu.VMEM((columns, slices, width, lanes), f32),
            pltpu.VMEM((slices, 8, lanes), f32),
            pltpu.VMEM((rounds, message, lanes), f32),
            pltpu.VMEM((rounds, n, message, lanes), f32),
            pltpu.VMEM((8, lanes), f32),
            pltpu.VMEM((nz, 8, lanes), f32),
            dma((per_col, 3, n)),
            dma((columns, 3)),
            dma((columns, pieces)),
            dma((columns, pieces)),
            dma((rounds, n)),
            dma((rounds, n)),
            dma((nz,)),
            dma((nz,)),
        ],
        compiler_params=pltpu.CompilerParams(
            collective_id=0, has_side_effects=True, vmem_limit_bytes=67_000_000
        ),
    )(layout.T, assign.T, edge, gate_left, gate_right, phase_angle, close)
    return amp.T, log.reshape(slices), total.reshape(2), top.reshape(())


def solution(mesh):
    in_specs = (
        P(None, "col"),
        P("cuts", "col"),
        P(),
        P("col", None, None, None),
        P("col", None, None, None),
        P(),
        P(),
    )
    out_specs = (P("cuts", None), P("cuts"), P(), P())
    return jax.shard_map(body, mesh=mesh, in_specs=in_specs, out_specs=out_specs, check_vma=False)
```

```python
import functools
import math

import jax
import jax.numpy as jnp
from jax import lax
from jax.experimental import pallas as pl
from jax.experimental.pallas import tpu as pltpu
from jax.sharding import PartitionSpec as P

MESH = pl.DeviceIdType.MESH
SEGMENT = 8


def split(value):
    high = value.astype(jnp.bfloat16)
    low = (value - high.astype(jnp.float32)).astype(jnp.bfloat16)
    return high, low


def swap(value, width):
    return pltpu.roll(value, width, len(value.shape) - 1)


def position(device, n):
    if n % 8:
        return device
    chip = lax.rem(device // 2, 4)
    return device + 2 * (chip // 2) * (1 - 2 * lax.rem(chip, 2))


device_at = position


def kernel(
    n, nz, rows,
    layout_ref, assign_ref, edge_hbm, left_hbm, right_hbm, angle_ref, close_hbm,
    result_ref,
    edge_ref, left_ref, right_ref, close_ref, cos_ref, sin_ref, load_sem, stage, stage_phase, gates, phases, board, halo, peak, xsend, xrecv, zsend, zrecv,
    gate_send, gate_recv, pass_send, halo_send, halo_recv, x_send, x_recv, z_send, z_recv,
):
    me = lax.axis_index("col")
    mz = lax.axis_index("cuts")
    per_col = left_ref.shape[0]
    columns = n * per_col
    own = rows // n
    slices = assign_ref.shape[1]
    pieces = 2 if slices % 2 == 0 else 1
    part_size = slices // pieces
    width = left_ref.shape[2]
    lanes = 2 * width
    place = position(me, n)
    last = place == n - 1
    next_row = jnp.minimum((place + 1) * own, rows - 1)
    loads = [
        pltpu.make_async_copy(left_hbm, left_ref, load_sem.at[0]),
        pltpu.make_async_copy(right_hbm, right_ref, load_sem.at[1]),
        pltpu.make_async_copy(
            edge_hbm.at[pl.ds(place * own, own)], edge_ref.at[pl.ds(0, own)], load_sem.at[2]
        ),
        pltpu.make_async_copy(
            edge_hbm.at[pl.ds(next_row, 1)], edge_ref.at[pl.ds(own, 1)], load_sem.at[3]
        ),
        pltpu.make_async_copy(close_hbm.at[pl.ds(place * own, own)], close_ref, load_sem.at[4]),
    ]
    for load in loads:
        load.start()

    barrier = pltpu.get_barrier_semaphore()
    for k in range(1, n):
        pl.semaphore_signal(
            barrier, inc=1, device_id=(lax.rem(me + k, n), mz), device_id_type=MESH
        )
    for k in range(1, nz):
        pl.semaphore_signal(
            barrier, inc=1, device_id=(me, lax.rem(mz + k, nz)), device_id_type=MESH
        )

    lane = lax.broadcasted_iota(jnp.int32, (1, lanes), 1)
    sign = jnp.where(lane < width, -1.0, 1.0).astype(jnp.float32)

    angle = angle_ref[...]
    cosine, sine = jnp.cos(angle), jnp.sin(angle)
    cos_ref[...] = jnp.concatenate([cosine, cosine], axis=1)
    sin_ref[...] = jnp.concatenate([-sine, sine], axis=1)
    for s in range(slices):
        peak[s] = jnp.ones(peak.shape[1:], jnp.float32)

    @pl.when(last)
    def _():
        halo[...] = jnp.zeros_like(halo)

    loads[0].wait()
    loads[1].wait()
    for cl in range(per_col):
        for s in range(slices):
            value = assign_ref[cl, s]
            stage_phase[cl, pl.ds(s, 1), :] = cos_ref[pl.ds(value, 1), :]
            stage_phase[cl, pl.ds(slices + s, 1), :] = sin_ref[pl.ds(value, 1), :]
        for r in range(rows):
            kind = layout_ref[cl, r]
            stage[cl, 0, r] = left_ref[cl, kind].astype(jnp.float32)
            stage[cl, 1, r] = right_ref[cl, kind].astype(jnp.float32)

    partner = mz + 1 - 2 * lax.rem(mz, 2) if nz % 2 == 0 else mz

    def direct(column, target):
        if nz % 2:
            return target >= 0
        near = (column // per_col) // 2 == target // 2
        return jnp.logical_or(near, lax.rem(column, 2) == lax.rem(mz, 2))

    def passes(column):
        if nz % 2:
            return me < 0
        far = (column // per_col) // 2 != me // 2
        return jnp.logical_and(far, lax.rem(column, 2) == lax.rem(mz, 2))

    def gate_copy(cl, part, target):
        column = me * per_col + cl
        if part == 2:
            source, sink = stage_phase.at[cl], phases.at[column]
        else:
            source = stage.at[cl, part, pl.ds(position(target, n) * own, own)]
            sink = gates.at[column, part]
        return pltpu.make_async_remote_copy(
            src_ref=source,
            dst_ref=sink,
            send_sem=gate_send.at[cl, part, target],
            recv_sem=gate_recv.at[column, part],
            device_id=(target, mz),
            device_id_type=MESH,
        )

    pl.semaphore_wait(barrier, n - 1 + nz - 1)
    for cl in range(per_col):
        for k in range(1, n):
            target = device_at(lax.rem(place + n - k, n), n)
            gate_copy(cl, 2, target).start()

            @pl.when(direct(me * per_col + cl, target))
            def _():
                gate_copy(cl, 0, target).start()
                gate_copy(cl, 1, target).start()
    for cl in range(per_col):
        column = me * per_col + cl
        phases[column] = stage_phase[cl]
        for part in range(2):
            gates[column, part] = stage[cl, part, pl.ds(place * own, own)]

    def pass_copy(column, part):
        return pltpu.make_async_remote_copy(
            src_ref=gates.at[column, part],
            dst_ref=gates.at[column, part],
            send_sem=pass_send.at[column, part],
            recv_sem=gate_recv.at[column, part],
            device_id=(me, partner),
            device_id_type=MESH,
        )

    def pass_on(column):
        @pl.when(passes(column))
        def _():
            for part in range(2):
                pass_copy(column, part).wait_recv()
                pass_copy(column, part).start()

    def wait_gates(column, part):
        sink = phases.at[column] if part == 2 else gates.at[column, part]
        needed = column // per_col != me
        if part < 2:
            needed = jnp.logical_and(needed, jnp.logical_not(passes(column)))

        @pl.when(needed)
        def _():
            pltpu.make_async_remote_copy(
                src_ref=sink,
                dst_ref=sink,
                send_sem=gate_send.at[0, part, 0],
                recv_sem=gate_recv.at[column, part],
                device_id=(lax.rem(me + 1, n), mz),
                device_id_type=MESH,
            ).wait_recv()

    def halo_copy(column, piece):
        part = pl.ds(piece * part_size, part_size)
        return pltpu.make_async_remote_copy(
            src_ref=board.at[column, 0, part],
            dst_ref=halo.at[column, part],
            send_sem=halo_send.at[column, piece],
            recv_sem=halo_recv.at[column, piece],
            device_id=(device_at(lax.rem(place + n - 1, n), n), mz),
            device_id_type=MESH,
        )

    def one_row(column, r, mixed, right_wait, send):
        left = gates[column, 0, r].astype(jnp.bfloat16)
        left = jnp.concatenate([left, left], axis=1)
        stacks = []
        for m in mixed:
            high, low = split(m)
            turned_high, turned_low = split(swap(m, width) * sign)
            stacks.append(jnp.concatenate([high, turned_high, low, turned_low], axis=0))
        middle = jnp.dot(
            left, jnp.concatenate(stacks, axis=1), preferred_element_type=jnp.float32
        )
        if right_wait:
            wait_gates(column, 1)
            wait_gates(column, 2)
        right = gates[column, 1, r]
        right = jnp.concatenate([right, swap(right, width) * sign], axis=0).astype(jnp.bfloat16)
        right = jnp.concatenate([right, right], axis=0)
        high, low = split(
            jnp.concatenate([middle[:, i * lanes:(i + 1) * lanes] for i in range(len(mixed))], axis=0)
        )
        outs = jnp.dot(
            jnp.concatenate([high, low], axis=1), right, preferred_element_type=jnp.float32
        )
        for s in range(slices):
            i = s if len(mixed) > 1 else 0
            out = outs[i * width:(i + 1) * width]
            if len(mixed) == 1 and s > 0:
                out_swapped = first_swapped
            else:
                out_swapped = swap(out, width)
                first_swapped = out_swapped
            turned = out * phases[column, pl.ds(s, 1), :] + out_swapped * phases[
                column, pl.ds(slices + s, 1), :
            ]
            board[column, r, s] = turned
            size = jnp.abs(turned).reshape(width // 8, 8, lanes)
            peak[s] = jnp.maximum(peak[s], jnp.max(size, axis=0))
            if send and (s + 1) % part_size == 0:
                @pl.when(place > 0)
                def _():
                    halo_copy(column, s // part_size).start()

    for load in loads[2:]:
        load.wait()
    for column in range(min(2, columns)):
        pass_on(column)
    wait_gates(0, 0)
    if columns > 2:
        pass_on(2)
    for r in range(own):
        below = edge_ref[r + 1].astype(jnp.float32)
        weight = 0.5 if r + 1 < own else jnp.where(last, 0.0, 0.5).astype(jnp.float32)
        mixed = edge_ref[r].astype(jnp.float32) + weight * below
        one_row(0, r, [mixed], r == 0, r == 0 and columns > 1)

    def column_step(column, scale, send):
        wait_gates(column, 0)

        @pl.when(column + 2 < columns)
        def _():
            pass_on(jnp.minimum(column + 2, columns - 1))
        for r in range(own):
            mixed = []
            for s in range(slices):
                if r + 1 == own and s % part_size == 0:
                    @pl.when(jnp.logical_not(last))
                    def _():
                        halo_copy(column - 1, s // part_size).wait_recv()
                below = board[column - 1, r + 1, s] if r + 1 < own else halo[column - 1, s]
                m = board[column - 1, r, s] + 0.5 * below
                mixed.append(m if scale is None else m * scale[s])
            one_row(column, r, mixed, r == 0, send and r == 0)

    def exchange(slot, count, index, axis_copy, sender, receiver):
        def copy(target):
            return axis_copy(slot, target)

        receiver[slot, index] = sender[slot]
        for k in range(1, count):
            copy(lax.rem(index + k, count)).start()
        for k in range(1, count):
            copy(lax.rem(index + k, count)).wait_send()

    def x_copy(slot, target):
        return pltpu.make_async_remote_copy(
            src_ref=xsend.at[slot],
            dst_ref=xrecv.at[slot, me],
            send_sem=x_send.at[slot, target],
            recv_sem=x_recv.at[slot, me],
            device_id=(target, mz),
            device_id_type=MESH,
        )

    def x_wait(slot):
        for k in range(1, n):
            source = lax.rem(me + k, n)
            pltpu.make_async_remote_copy(
                src_ref=xsend.at[slot],
                dst_ref=xrecv.at[slot, source],
                send_sem=x_send.at[slot, source],
                recv_sem=x_recv.at[slot, source],
                device_id=(source, mz),
                device_id_type=MESH,
            ).wait_recv()

    def z_copy(target):
        return pltpu.make_async_remote_copy(
            src_ref=zsend,
            dst_ref=zrecv.at[mz],
            send_sem=z_send.at[target],
            recv_sem=z_recv.at[mz],
            device_id=(me, target),
            device_id_type=MESH,
        )

    def local_peaks():
        return [
            jnp.max(jnp.max(peak[s], axis=0, keepdims=True), axis=1, keepdims=True)
            for s in range(slices)
        ]

    logs = [jnp.zeros((1, 1), jnp.float32)] * slices
    scale = None
    begin, slot = 1, 0
    while True:
        stop = min(columns, (begin // SEGMENT + 1) * SEGMENT)
        if scale is not None:
            column_step(begin, scale, begin + 1 < columns)
            begin += 1
        full = min(stop, columns - 1)

        def loop_step(column, carry):
            column_step(column, None, True)
            return carry

        if full > begin:
            lax.fori_loop(begin, full, loop_step, 0)
        if stop == columns:
            if columns - 1 >= begin:
                column_step(columns - 1, None, False)
            break
        for s, m in enumerate(local_peaks()):
            xsend[slot, pl.ds(s, 1), :] = jnp.broadcast_to(m, (1, lanes))
        exchange(slot, n, me, x_copy, xsend, xrecv)
        x_wait(slot)
        scale = []
        for s in range(slices):
            m = xrecv[slot, 0, pl.ds(s, 1), :]
            for d in range(1, n):
                m = jnp.maximum(m, xrecv[slot, d, pl.ds(s, 1), :])
            logs[s] = logs[s] + jnp.log(m[:, :1])
            scale.append(1.0 / m)
            peak[s] = jnp.ones(peak.shape[1:], jnp.float32)
        begin, slot = stop, slot + 1

    factor = 1.0 / math.sqrt(rows * width * width)
    mine = local_peaks()
    for s in range(slices):
        real = jnp.zeros((8, lanes), jnp.float32)
        imag = jnp.zeros((8, lanes), jnp.float32)
        inverse = 1.0 / mine[s]
        for r in range(own):
            close = close_ref[r]
            value = board[columns - 1, r, s] * inverse
            real = real + jnp.sum((value * close).reshape(width // 8, 8, lanes), axis=0)
            imag = imag + jnp.sum((value * swap(close, width)).reshape(width // 8, 8, lanes), axis=0)
        xsend[slot, pl.ds(s, 1), :] = jnp.sum(real, axis=0, keepdims=True) * (-sign)
        xsend[slot, pl.ds(slices + s, 1), :] = jnp.sum(imag, axis=0, keepdims=True)
        xsend[slot, pl.ds(2 * slices + s, 1), :] = jnp.broadcast_to(mine[s], (1, lanes))
    exchange(slot, n, me, x_copy, xsend, xrecv)
    x_wait(slot)
    all_peaks = [xrecv[slot, d, pl.ds(2 * slices, slices), :] for d in range(n)]
    top_peak = functools.reduce(jnp.maximum, all_peaks)
    inverse = 1.0 / top_peak
    real = jnp.zeros((slices, lanes), jnp.float32)
    imag = jnp.zeros((slices, lanes), jnp.float32)
    for d in range(n):
        ratio = all_peaks[d] * inverse
        real = real + xrecv[slot, d, pl.ds(0, slices), :] * ratio
        imag = imag + xrecv[slot, d, pl.ds(slices, slices), :] * ratio
    real = jnp.sum(real, axis=1, keepdims=True) * factor
    imag = jnp.sum(imag, axis=1, keepdims=True) * factor
    log = jnp.log(top_peak)[:, :1] + jnp.concatenate(logs, axis=0)
    result_ref[pl.ds(0, slices), :] = jnp.where(lane == 0, real, jnp.where(lane == 1, imag, log))
    top = jnp.max(log, axis=0, keepdims=True)
    share = jnp.exp(log - top)
    zsend[pl.ds(0, 1), :] = jnp.broadcast_to(jnp.sum(real * share, axis=0, keepdims=True), (1, lanes))
    zsend[pl.ds(1, 1), :] = jnp.broadcast_to(jnp.sum(imag * share, axis=0, keepdims=True), (1, lanes))
    zsend[pl.ds(2, 1), :] = jnp.broadcast_to(top, (1, lanes))
    zrecv[mz] = zsend[...]
    for k in range(1, nz):
        z_copy(lax.rem(mz + k, nz)).start()
    for k in range(1, nz):
        source = lax.rem(mz + k, nz)
        pltpu.make_async_remote_copy(
            src_ref=zsend,
            dst_ref=zrecv.at[source],
            send_sem=z_send.at[source],
            recv_sem=z_recv.at[source],
            device_id=(me, source),
            device_id_type=MESH,
        ).wait_recv()
    tops = [zrecv[z, pl.ds(2, 1), :] for z in range(nz)]
    top = functools.reduce(jnp.maximum, tops)
    real = jnp.zeros((1, lanes), jnp.float32)
    imag = jnp.zeros((1, lanes), jnp.float32)
    for z in range(nz):
        share = jnp.exp(tops[z] - top)
        real = real + zrecv[z, pl.ds(0, 1), :] * share
        imag = imag + zrecv[z, pl.ds(1, 1), :] * share
    result_ref[pl.ds(slices, 1), :] = jnp.where(lane == 0, real, jnp.where(lane == 1, imag, top))

    for k in range(1, nz):
        z_copy(lax.rem(mz + k, nz)).wait_send()
    for cl in range(per_col):
        for k in range(1, n):
            target = lax.rem(me + k, n)
            gate_copy(cl, 2, target).wait_send()

            @pl.when(direct(me * per_col + cl, target))
            def _():
                gate_copy(cl, 0, target).wait_send()
                gate_copy(cl, 1, target).wait_send()
    for column in range(columns):
        @pl.when(passes(column))
        def _():
            pass_copy(column, 0).wait_send()
            pass_copy(column, 1).wait_send()
    if columns > 1:
        @pl.when(place > 0)
        def _():
            for column in range(columns - 1):
                for piece in range(pieces):
                    halo_copy(column, piece).wait_send()


def unpack(result_ref, amp_ref, log_ref, total_ref, top_ref):
    slices = amp_ref.shape[1]
    for s in range(slices):
        for k in range(2):
            amp_ref[pl.ds(k, 1), pl.ds(s, 1)] = result_ref[pl.ds(s, 1), pl.ds(k, 1)]
        log_ref[:, pl.ds(s, 1)] = result_ref[pl.ds(s, 1), pl.ds(2, 1)]
    total_ref[...] = result_ref[pl.ds(slices, 1), pl.ds(0, 2)]
    top_ref[...] = result_ref[pl.ds(slices, 1), pl.ds(2, 1)]


def body(layout, assign, edge, gate_left, gate_right, phase_angle, close):
    n, nz = lax.axis_size("col"), lax.axis_size("cuts")
    rows, width, lanes = edge.shape
    per_col = gate_left.shape[0]
    columns, own, slices = n * per_col, rows // n, assign.shape[0]
    rounds = -(-columns // SEGMENT)
    pieces = 2 if slices % 2 == 0 else 1
    f32 = jnp.float32
    vmem = pl.BlockSpec(memory_space=pltpu.VMEM)
    hbm = pl.BlockSpec(memory_space=pltpu.HBM)
    smem = pl.BlockSpec(memory_space=pltpu.SMEM)
    dma = pltpu.SemaphoreType.DMA
    message = -(-3 * slices // 8) * 8
    phase_rows = -(-2 * slices // 8) * 8
    result = pl.pallas_call(
        functools.partial(kernel, n, nz, rows),
        out_shape=jax.ShapeDtypeStruct((-(-(slices + 1) // 8) * 8, lanes), f32),
        in_specs=[smem, smem, hbm, hbm, hbm, vmem, hbm],
        out_specs=vmem,
        scratch_shapes=[
            pltpu.VMEM((own + 1, width, lanes), edge.dtype),
            pltpu.VMEM(gate_left.shape, gate_left.dtype),
            pltpu.VMEM(gate_right.shape, gate_right.dtype),
            pltpu.VMEM((own, width, lanes), f32),
            pltpu.VMEM((phase_angle.shape[0], lanes), f32),
            pltpu.VMEM((phase_angle.shape[0], lanes), f32),
            dma((5,)),
            pltpu.VMEM((per_col, 2, rows, width, lanes), f32),
            pltpu.VMEM((per_col, phase_rows, lanes), f32),
            pltpu.VMEM((columns, 2, own, width, lanes), f32),
            pltpu.VMEM((columns, phase_rows, lanes), f32),
            pltpu.VMEM((columns, own, slices, width, lanes), f32),
            pltpu.VMEM((columns, slices, width, lanes), f32),
            pltpu.VMEM((slices, 8, lanes), f32),
            pltpu.VMEM((rounds, message, lanes), f32),
            pltpu.VMEM((rounds, n, message, lanes), f32),
            pltpu.VMEM((8, lanes), f32),
            pltpu.VMEM((nz, 8, lanes), f32),
            dma((per_col, 3, n)),
            dma((columns, 3)),
            dma((columns, 2)),
            dma((columns, pieces)),
            dma((columns, pieces)),
            dma((rounds, n)),
            dma((rounds, n)),
            dma((nz,)),
            dma((nz,)),
        ],
        compiler_params=pltpu.CompilerParams(
            collective_id=0, has_side_effects=True, vmem_limit_bytes=67_000_000
        ),
    )(layout.T, assign.T, edge, gate_left, gate_right, phase_angle, close)
    amp, log, total, top = pl.pallas_call(
        unpack,
        out_shape=[
            jax.ShapeDtypeStruct((2, slices), f32),
            jax.ShapeDtypeStruct((1, slices), f32),
            jax.ShapeDtypeStruct((1, 2), f32),
            jax.ShapeDtypeStruct((1, 1), f32),
        ],
        in_specs=[vmem],
        out_specs=[vmem] * 4,
    )(result)
    return amp.T, log.reshape(slices), total.reshape(2), top.reshape(())


def solution(mesh):
    in_specs = (
        P(None, "col"),
        P("cuts", "col"),
        P(),
        P("col", None, None, None),
        P("col", None, None, None),
        P(),
        P(),
    )
    out_specs = (P("cuts", None), P("cuts"), P(), P())
    return jax.shard_map(body, mesh=mesh, in_specs=in_specs, out_specs=out_specs, check_vma=False)
```

```python
import functools
import math

import jax
import jax.numpy as jnp
from jax import lax
from jax.experimental import pallas as pl
from jax.experimental.pallas import tpu as pltpu
from jax.sharding import PartitionSpec as P

MESH = pl.DeviceIdType.MESH
SEGMENT = 8


def split(value):
    high = value.astype(jnp.bfloat16)
    low = (value - high.astype(jnp.float32)).astype(jnp.bfloat16)
    return high, low


def swap(value, width):
    return pltpu.roll(value, width, len(value.shape) - 1)


def position(device, n):
    if n % 8:
        return device
    chip = lax.rem(device // 2, 4)
    return device + 2 * (chip // 2) * (1 - 2 * lax.rem(chip, 2))


device_at = position


def kernel(
    n, nz, rows,
    layout_ref, assign_ref, edge_hbm, left_hbm, right_hbm, angle_ref, close_hbm,
    result_ref,
    edge_ref, left_ref, right_ref, close_ref, cos_ref, sin_ref, load_sem, stage, stage_phase, gates, phases, board, halo, peak, xsend, xrecv, zsend, zrecv,
    gate_send, gate_recv, pass_send, halo_send, halo_recv, x_send, x_recv, z_send, z_recv,
):
    me = lax.axis_index("col")
    mz = lax.axis_index("cuts")
    per_col = left_ref.shape[0]
    columns = n * per_col
    own = rows // n
    slices = assign_ref.shape[1]
    pieces = 2 if slices % 2 == 0 else 1
    part_size = slices // pieces
    width = left_ref.shape[2]
    lanes = 2 * width
    place = position(me, n)
    last = place == n - 1
    next_row = jnp.minimum((place + 1) * own, rows - 1)
    loads = [
        pltpu.make_async_copy(left_hbm, left_ref, load_sem.at[0]),
        pltpu.make_async_copy(right_hbm, right_ref, load_sem.at[1]),
        pltpu.make_async_copy(
            edge_hbm.at[pl.ds(place * own, own)], edge_ref.at[pl.ds(0, own)], load_sem.at[2]
        ),
        pltpu.make_async_copy(
            edge_hbm.at[pl.ds(next_row, 1)], edge_ref.at[pl.ds(own, 1)], load_sem.at[3]
        ),
        pltpu.make_async_copy(close_hbm.at[pl.ds(place * own, own)], close_ref, load_sem.at[4]),
    ]
    for load in loads:
        load.start()

    barrier = pltpu.get_barrier_semaphore()
    for k in range(1, n):
        pl.semaphore_signal(
            barrier, inc=1, device_id=(lax.rem(me + k, n), mz), device_id_type=MESH
        )
    for k in range(1, nz):
        pl.semaphore_signal(
            barrier, inc=1, device_id=(me, lax.rem(mz + k, nz)), device_id_type=MESH
        )

    lane = lax.broadcasted_iota(jnp.int32, (1, lanes), 1)
    sign = jnp.where(lane < width, -1.0, 1.0).astype(jnp.float32)

    angle = angle_ref[...]
    cosine, sine = jnp.cos(angle), jnp.sin(angle)
    cos_ref[...] = jnp.concatenate([cosine, cosine], axis=1)
    sin_ref[...] = jnp.concatenate([-sine, sine], axis=1)
    for s in range(slices):
        peak[s] = jnp.ones(peak.shape[1:], jnp.float32)

    @pl.when(last)
    def _():
        halo[...] = jnp.zeros_like(halo)

    loads[0].wait()
    loads[1].wait()
    for cl in range(per_col):
        for s in range(slices):
            value = assign_ref[cl, s]
            stage_phase[cl, pl.ds(s, 1), :] = cos_ref[pl.ds(value, 1), :]
            stage_phase[cl, pl.ds(slices + s, 1), :] = sin_ref[pl.ds(value, 1), :]
        for r in range(rows):
            kind = layout_ref[cl, r]
            stage[cl, 0, r] = left_ref[cl, kind].astype(jnp.float32)
            stage[cl, 1, r] = right_ref[cl, kind].astype(jnp.float32)

    partner = mz + 1 - 2 * lax.rem(mz, 2) if nz % 2 == 0 else mz

    def direct(column, target):
        if nz % 2:
            return target >= 0
        near = (column // per_col) // 2 == target // 2
        return jnp.logical_or(near, lax.rem(column, 2) == lax.rem(mz, 2))

    def passes(column):
        if nz % 2:
            return me < 0
        far = (column // per_col) // 2 != me // 2
        return jnp.logical_and(far, lax.rem(column, 2) == lax.rem(mz, 2))

    def gate_copy(cl, part, target):
        column = me * per_col + cl
        if part == 2:
            source, sink = stage_phase.at[cl], phases.at[column]
        else:
            source = stage.at[cl, part, pl.ds(position(target, n) * own, own)]
            sink = gates.at[column, part]
        return pltpu.make_async_remote_copy(
            src_ref=source,
            dst_ref=sink,
            send_sem=gate_send.at[cl, part, target],
            recv_sem=gate_recv.at[column, part],
            device_id=(target, mz),
            device_id_type=MESH,
        )

    pl.semaphore_wait(barrier, n - 1 + nz - 1)
    for cl in range(per_col):
        for k in range(1, n):
            target = device_at(lax.rem(place + n - k, n), n)
            gate_copy(cl, 2, target).start()

            @pl.when(direct(me * per_col + cl, target))
            def _():
                gate_copy(cl, 0, target).start()
                gate_copy(cl, 1, target).start()
    for cl in range(per_col):
        column = me * per_col + cl
        phases[column] = stage_phase[cl]
        for part in range(2):
            gates[column, part] = stage[cl, part, pl.ds(place * own, own)]

    def pass_copy(column, part):
        return pltpu.make_async_remote_copy(
            src_ref=gates.at[column, part],
            dst_ref=gates.at[column, part],
            send_sem=pass_send.at[column, part],
            recv_sem=gate_recv.at[column, part],
            device_id=(me, partner),
            device_id_type=MESH,
        )

    def pass_on(column):
        @pl.when(passes(column))
        def _():
            for part in range(2):
                pass_copy(column, part).wait_recv()
                pass_copy(column, part).start()

    def wait_gates(column, part):
        sink = phases.at[column] if part == 2 else gates.at[column, part]
        needed = column // per_col != me
        if part < 2:
            needed = jnp.logical_and(needed, jnp.logical_not(passes(column)))

        @pl.when(needed)
        def _():
            pltpu.make_async_remote_copy(
                src_ref=sink,
                dst_ref=sink,
                send_sem=gate_send.at[0, part, 0],
                recv_sem=gate_recv.at[column, part],
                device_id=(lax.rem(me + 1, n), mz),
                device_id_type=MESH,
            ).wait_recv()

    def halo_copy(column, piece):
        part = pl.ds(piece * part_size, part_size)
        return pltpu.make_async_remote_copy(
            src_ref=board.at[column, 0, part],
            dst_ref=halo.at[column, part],
            send_sem=halo_send.at[column, piece],
            recv_sem=halo_recv.at[column, piece],
            device_id=(device_at(lax.rem(place + n - 1, n), n), mz),
            device_id_type=MESH,
        )

    def one_row(column, r, mixed, right_wait, send):
        left = gates[column, 0, r].astype(jnp.bfloat16)
        left = jnp.concatenate([left, left], axis=1)
        stacks = []
        for m in mixed:
            high, low = split(m)
            turned_high, turned_low = split(swap(m, width) * sign)
            stacks.append(jnp.concatenate([high, turned_high, low, turned_low], axis=0))
        middle = jnp.dot(
            left, jnp.concatenate(stacks, axis=1), preferred_element_type=jnp.float32
        )
        if right_wait:
            wait_gates(column, 1)
            wait_gates(column, 2)
        right = gates[column, 1, r]
        right = jnp.concatenate([right, swap(right, width) * sign], axis=0).astype(jnp.bfloat16)
        right = jnp.concatenate([right, right], axis=0)
        high, low = split(
            jnp.concatenate([middle[:, i * lanes:(i + 1) * lanes] for i in range(len(mixed))], axis=0)
        )
        outs = jnp.dot(
            jnp.concatenate([high, low], axis=1), right, preferred_element_type=jnp.float32
        )
        for s in range(slices):
            i = s if len(mixed) > 1 else 0
            out = outs[i * width:(i + 1) * width]
            if len(mixed) == 1 and s > 0:
                out_swapped = first_swapped
            else:
                out_swapped = swap(out, width)
                first_swapped = out_swapped
            turned = out * phases[column, pl.ds(s, 1), :] + out_swapped * phases[
                column, pl.ds(slices + s, 1), :
            ]
            board[column, r, s] = turned
            size = jnp.abs(turned).reshape(width // 8, 8, lanes)
            peak[s] = jnp.maximum(peak[s], jnp.max(size, axis=0))
            if send and (s + 1) % part_size == 0:
                @pl.when(place > 0)
                def _():
                    halo_copy(column, s // part_size).start()

    for load in loads[2:]:
        load.wait()
    for column in range(min(2, columns)):
        pass_on(column)
    wait_gates(0, 0)
    for r in range(own):
        below = edge_ref[r + 1].astype(jnp.float32)
        weight = 0.5 if r + 1 < own else jnp.where(last, 0.0, 0.5).astype(jnp.float32)
        mixed = edge_ref[r].astype(jnp.float32) + weight * below
        one_row(0, r, [mixed], r == 0, r == 0 and columns > 1)
        if r == 0 and columns > 2:
            pass_on(2)

    def column_step(column, scale, send):
        for part in range(3):
            wait_gates(column, part)
        for r in range(own):
            mixed = []
            for s in range(slices):
                if r + 1 == own and s % part_size == 0:
                    @pl.when(jnp.logical_not(last))
                    def _():
                        halo_copy(column - 1, s // part_size).wait_recv()
                below = board[column - 1, r + 1, s] if r + 1 < own else halo[column - 1, s]
                m = board[column - 1, r, s] + 0.5 * below
                mixed.append(m if scale is None else m * scale[s])
            one_row(column, r, mixed, False, send and r == 0)
            if r == 0:
                @pl.when(column + 2 < columns)
                def _():
                    pass_on(jnp.minimum(column + 2, columns - 1))

    def exchange(slot, count, index, axis_copy, sender, receiver):
        def copy(target):
            return axis_copy(slot, target)

        receiver[slot, index] = sender[slot]
        for k in range(1, count):
            copy(lax.rem(index + k, count)).start()
        for k in range(1, count):
            copy(lax.rem(index + k, count)).wait_send()

    def x_copy(slot, target):
        return pltpu.make_async_remote_copy(
            src_ref=xsend.at[slot],
            dst_ref=xrecv.at[slot, me],
            send_sem=x_send.at[slot, target],
            recv_sem=x_recv.at[slot, me],
            device_id=(target, mz),
            device_id_type=MESH,
        )

    def x_wait(slot):
        for k in range(1, n):
            source = lax.rem(me + k, n)
            pltpu.make_async_remote_copy(
                src_ref=xsend.at[slot],
                dst_ref=xrecv.at[slot, source],
                send_sem=x_send.at[slot, source],
                recv_sem=x_recv.at[slot, source],
                device_id=(source, mz),
                device_id_type=MESH,
            ).wait_recv()

    def z_copy(target):
        return pltpu.make_async_remote_copy(
            src_ref=zsend,
            dst_ref=zrecv.at[mz],
            send_sem=z_send.at[target],
            recv_sem=z_recv.at[mz],
            device_id=(me, target),
            device_id_type=MESH,
        )

    def local_peaks():
        return [
            jnp.max(jnp.max(peak[s], axis=0, keepdims=True), axis=1, keepdims=True)
            for s in range(slices)
        ]

    logs = [jnp.zeros((1, 1), jnp.float32)] * slices
    scale = None
    begin, slot = 1, 0
    while True:
        stop = min(columns, (begin // SEGMENT + 1) * SEGMENT)
        if scale is not None:
            column_step(begin, scale, begin + 1 < columns)
            begin += 1
        full = min(stop, columns - 1)

        def loop_step(column, carry):
            column_step(column, None, True)
            return carry

        if full > begin:
            lax.fori_loop(begin, full, loop_step, 0)
        if stop == columns:
            if columns - 1 >= begin:
                column_step(columns - 1, None, False)
            break
        for s, m in enumerate(local_peaks()):
            xsend[slot, pl.ds(s, 1), :] = jnp.broadcast_to(m, (1, lanes))
        exchange(slot, n, me, x_copy, xsend, xrecv)
        x_wait(slot)
        scale = []
        for s in range(slices):
            m = xrecv[slot, 0, pl.ds(s, 1), :]
            for d in range(1, n):
                m = jnp.maximum(m, xrecv[slot, d, pl.ds(s, 1), :])
            logs[s] = logs[s] + jnp.log(m[:, :1])
            scale.append(1.0 / m)
            peak[s] = jnp.ones(peak.shape[1:], jnp.float32)
        begin, slot = stop, slot + 1

    factor = 1.0 / math.sqrt(rows * width * width)
    mine = local_peaks()
    for s in range(slices):
        real = jnp.zeros((8, lanes), jnp.float32)
        imag = jnp.zeros((8, lanes), jnp.float32)
        inverse = 1.0 / mine[s]
        for r in range(own):
            close = close_ref[r]
            value = board[columns - 1, r, s] * inverse
            real = real + jnp.sum((value * close).reshape(width // 8, 8, lanes), axis=0)
            imag = imag + jnp.sum((value * swap(close, width)).reshape(width // 8, 8, lanes), axis=0)
        xsend[slot, pl.ds(s, 1), :] = jnp.sum(real, axis=0, keepdims=True) * (-sign)
        xsend[slot, pl.ds(slices + s, 1), :] = jnp.sum(imag, axis=0, keepdims=True)
        xsend[slot, pl.ds(2 * slices + s, 1), :] = jnp.broadcast_to(mine[s], (1, lanes))
    exchange(slot, n, me, x_copy, xsend, xrecv)
    x_wait(slot)
    all_peaks = [xrecv[slot, d, pl.ds(2 * slices, slices), :] for d in range(n)]
    top_peak = functools.reduce(jnp.maximum, all_peaks)
    inverse = 1.0 / top_peak
    real = jnp.zeros((slices, lanes), jnp.float32)
    imag = jnp.zeros((slices, lanes), jnp.float32)
    for d in range(n):
        ratio = all_peaks[d] * inverse
        real = real + xrecv[slot, d, pl.ds(0, slices), :] * ratio
        imag = imag + xrecv[slot, d, pl.ds(slices, slices), :] * ratio
    real = jnp.sum(real, axis=1, keepdims=True) * factor
    imag = jnp.sum(imag, axis=1, keepdims=True) * factor
    log = jnp.log(top_peak)[:, :1] + jnp.concatenate(logs, axis=0)
    result_ref[pl.ds(0, slices), :] = jnp.where(lane == 0, real, jnp.where(lane == 1, imag, log))
    top = jnp.max(log, axis=0, keepdims=True)
    share = jnp.exp(log - top)
    zsend[pl.ds(0, 1), :] = jnp.broadcast_to(jnp.sum(real * share, axis=0, keepdims=True), (1, lanes))
    zsend[pl.ds(1, 1), :] = jnp.broadcast_to(jnp.sum(imag * share, axis=0, keepdims=True), (1, lanes))
    zsend[pl.ds(2, 1), :] = jnp.broadcast_to(top, (1, lanes))
    zrecv[mz] = zsend[...]
    for k in range(1, nz):
        z_copy(lax.rem(mz + k, nz)).start()
    for k in range(1, nz):
        source = lax.rem(mz + k, nz)
        pltpu.make_async_remote_copy(
            src_ref=zsend,
            dst_ref=zrecv.at[source],
            send_sem=z_send.at[source],
            recv_sem=z_recv.at[source],
            device_id=(me, source),
            device_id_type=MESH,
        ).wait_recv()
    tops = [zrecv[z, pl.ds(2, 1), :] for z in range(nz)]
    top = functools.reduce(jnp.maximum, tops)
    real = jnp.zeros((1, lanes), jnp.float32)
    imag = jnp.zeros((1, lanes), jnp.float32)
    for z in range(nz):
        share = jnp.exp(tops[z] - top)
        real = real + zrecv[z, pl.ds(0, 1), :] * share
        imag = imag + zrecv[z, pl.ds(1, 1), :] * share
    result_ref[pl.ds(slices, 1), :] = jnp.where(lane == 0, real, jnp.where(lane == 1, imag, top))

    for k in range(1, nz):
        z_copy(lax.rem(mz + k, nz)).wait_send()
    for cl in range(per_col):
        for k in range(1, n):
            target = lax.rem(me + k, n)
            gate_copy(cl, 2, target).wait_send()

            @pl.when(direct(me * per_col + cl, target))
            def _():
                gate_copy(cl, 0, target).wait_send()
                gate_copy(cl, 1, target).wait_send()
    for column in range(columns):
        @pl.when(passes(column))
        def _():
            pass_copy(column, 0).wait_send()
            pass_copy(column, 1).wait_send()
    if columns > 1:
        @pl.when(place > 0)
        def _():
            for column in range(columns - 1):
                for piece in range(pieces):
                    halo_copy(column, piece).wait_send()


def unpack(result_ref, amp_ref, log_ref, total_ref, top_ref):
    slices = amp_ref.shape[1]
    for s in range(slices):
        for k in range(2):
            amp_ref[pl.ds(k, 1), pl.ds(s, 1)] = result_ref[pl.ds(s, 1), pl.ds(k, 1)]
        log_ref[:, pl.ds(s, 1)] = result_ref[pl.ds(s, 1), pl.ds(2, 1)]
    total_ref[...] = result_ref[pl.ds(slices, 1), pl.ds(0, 2)]
    top_ref[...] = result_ref[pl.ds(slices, 1), pl.ds(2, 1)]


def body(layout, assign, edge, gate_left, gate_right, phase_angle, close):
    n, nz = lax.axis_size("col"), lax.axis_size("cuts")
    rows, width, lanes = edge.shape
    per_col = gate_left.shape[0]
    columns, own, slices = n * per_col, rows // n, assign.shape[0]
    rounds = -(-columns // SEGMENT)
    pieces = 2 if slices % 2 == 0 else 1
    f32 = jnp.float32
    vmem = pl.BlockSpec(memory_space=pltpu.VMEM)
    hbm = pl.BlockSpec(memory_space=pltpu.HBM)
    smem = pl.BlockSpec(memory_space=pltpu.SMEM)
    dma = pltpu.SemaphoreType.DMA
    message = -(-3 * slices // 8) * 8
    phase_rows = -(-2 * slices // 8) * 8
    result = pl.pallas_call(
        functools.partial(kernel, n, nz, rows),
        out_shape=jax.ShapeDtypeStruct((-(-(slices + 1) // 8) * 8, lanes), f32),
        in_specs=[smem, smem, hbm, hbm, hbm, vmem, hbm],
        out_specs=vmem,
        scratch_shapes=[
            pltpu.VMEM((own + 1, width, lanes), edge.dtype),
            pltpu.VMEM(gate_left.shape, gate_left.dtype),
            pltpu.VMEM(gate_right.shape, gate_right.dtype),
            pltpu.VMEM((own, width, lanes), f32),
            pltpu.VMEM((phase_angle.shape[0], lanes), f32),
            pltpu.VMEM((phase_angle.shape[0], lanes), f32),
            dma((5,)),
            pltpu.VMEM((per_col, 2, rows, width, lanes), f32),
            pltpu.VMEM((per_col, phase_rows, lanes), f32),
            pltpu.VMEM((columns, 2, own, width, lanes), f32),
            pltpu.VMEM((columns, phase_rows, lanes), f32),
            pltpu.VMEM((columns, own, slices, width, lanes), f32),
            pltpu.VMEM((columns, slices, width, lanes), f32),
            pltpu.VMEM((slices, 8, lanes), f32),
            pltpu.VMEM((rounds, message, lanes), f32),
            pltpu.VMEM((rounds, n, message, lanes), f32),
            pltpu.VMEM((8, lanes), f32),
            pltpu.VMEM((nz, 8, lanes), f32),
            dma((per_col, 3, n)),
            dma((columns, 3)),
            dma((columns, 2)),
            dma((columns, pieces)),
            dma((columns, pieces)),
            dma((rounds, n)),
            dma((rounds, n)),
            dma((nz,)),
            dma((nz,)),
        ],
        compiler_params=pltpu.CompilerParams(
            collective_id=0, has_side_effects=True, vmem_limit_bytes=67_000_000
        ),
    )(layout.T, assign.T, edge, gate_left, gate_right, phase_angle, close)
    amp, log, total, top = pl.pallas_call(
        unpack,
        out_shape=[
            jax.ShapeDtypeStruct((2, slices), f32),
            jax.ShapeDtypeStruct((1, slices), f32),
            jax.ShapeDtypeStruct((1, 2), f32),
            jax.ShapeDtypeStruct((1, 1), f32),
        ],
        in_specs=[vmem],
        out_specs=[vmem] * 4,
    )(result)
    return amp.T, log.reshape(slices), total.reshape(2), top.reshape(())


def solution(mesh):
    in_specs = (
        P(None, "col"),
        P("cuts", "col"),
        P(),
        P("col", None, None, None),
        P("col", None, None, None),
        P(),
        P(),
    )
    out_specs = (P("cuts", None), P("cuts"), P(), P())
    return jax.shard_map(body, mesh=mesh, in_specs=in_specs, out_specs=out_specs, check_vma=False)
```

```python
import functools
import math

import jax
import jax.numpy as jnp
from jax import lax
from jax.experimental import pallas as pl
from jax.experimental.pallas import tpu as pltpu
from jax.sharding import PartitionSpec as P

MESH = pl.DeviceIdType.MESH
SEGMENT = 8


def split(value):
    high = value.astype(jnp.bfloat16)
    low = (value - high.astype(jnp.float32)).astype(jnp.bfloat16)
    return high, low


def swap(value, width):
    return pltpu.roll(value, width, len(value.shape) - 1)


def position(device, n):
    if n % 8:
        return device
    chip = lax.rem(device // 2, 4)
    return device + 2 * (chip // 2) * (1 - 2 * lax.rem(chip, 2))


device_at = position


def kernel(
    n, nz, rows,
    layout_ref, assign_ref, edge_hbm, left_hbm, right_hbm, angle_ref, close_hbm,
    result_ref,
    edge_ref, left_ref, right_ref, close_ref, cos_ref, sin_ref, load_sem, stage, stage_phase, gates, phases, board, halo, peak, xsend, xrecv, zsend, zrecv,
    gate_send, gate_recv, pass_send, halo_send, halo_recv, x_send, x_recv, z_send, z_recv,
):
    me = lax.axis_index("col")
    mz = lax.axis_index("cuts")
    per_col = left_ref.shape[0]
    columns = n * per_col
    own = rows // n
    slices = assign_ref.shape[1]
    pieces = 2 if slices % 2 == 0 else 1
    part_size = slices // pieces
    width = left_ref.shape[2]
    lanes = 2 * width
    place = position(me, n)
    last = place == n - 1
    next_row = jnp.minimum((place + 1) * own, rows - 1)
    loads = [
        pltpu.make_async_copy(left_hbm, left_ref, load_sem.at[0]),
        pltpu.make_async_copy(right_hbm, right_ref, load_sem.at[1]),
        pltpu.make_async_copy(
            edge_hbm.at[pl.ds(place * own, own)], edge_ref.at[pl.ds(0, own)], load_sem.at[2]
        ),
        pltpu.make_async_copy(
            edge_hbm.at[pl.ds(next_row, 1)], edge_ref.at[pl.ds(own, 1)], load_sem.at[3]
        ),
        pltpu.make_async_copy(close_hbm.at[pl.ds(place * own, own)], close_ref, load_sem.at[4]),
    ]
    for load in loads:
        load.start()

    barrier = pltpu.get_barrier_semaphore()
    for k in range(1, n):
        pl.semaphore_signal(
            barrier, inc=1, device_id=(lax.rem(me + k, n), mz), device_id_type=MESH
        )
    for k in range(1, nz):
        pl.semaphore_signal(
            barrier, inc=1, device_id=(me, lax.rem(mz + k, nz)), device_id_type=MESH
        )

    lane = lax.broadcasted_iota(jnp.int32, (1, lanes), 1)
    sign = jnp.where(lane < width, -1.0, 1.0).astype(jnp.float32)

    angle = angle_ref[...]
    cosine, sine = jnp.cos(angle), jnp.sin(angle)
    cos_ref[...] = jnp.concatenate([cosine, cosine], axis=1)
    sin_ref[...] = jnp.concatenate([-sine, sine], axis=1)
    for s in range(slices):
        peak[s] = jnp.ones(peak.shape[1:], jnp.float32)

    @pl.when(last)
    def _():
        halo[...] = jnp.zeros_like(halo)

    loads[0].wait()
    loads[1].wait()
    for cl in range(per_col):
        for s in range(slices):
            value = assign_ref[cl, s]
            stage_phase[cl, pl.ds(s, 1), :] = cos_ref[pl.ds(value, 1), :]
            stage_phase[cl, pl.ds(slices + s, 1), :] = sin_ref[pl.ds(value, 1), :]
        for r in range(rows):
            kind = layout_ref[cl, r]
            stage[cl, 0, r] = left_ref[cl, kind].astype(jnp.float32)
            stage[cl, 1, r] = right_ref[cl, kind].astype(jnp.float32)

    partner = mz + 1 - 2 * lax.rem(mz, 2) if nz % 2 == 0 else mz

    def direct(column, target, part):
        if nz % 2:
            return target >= 0
        near = (column // per_col) // 2 == target // 2
        return jnp.logical_or(near, part == lax.rem(mz, 2))

    def passes(column, part):
        if nz % 2:
            return me < 0
        far = (column // per_col) // 2 != me // 2
        return jnp.logical_and(far, part == lax.rem(mz, 2))

    def gate_copy(cl, part, target):
        column = me * per_col + cl
        if part == 2:
            source, sink = stage_phase.at[cl], phases.at[column]
        else:
            source = stage.at[cl, part, pl.ds(position(target, n) * own, own)]
            sink = gates.at[column, part]
        return pltpu.make_async_remote_copy(
            src_ref=source,
            dst_ref=sink,
            send_sem=gate_send.at[cl, part, target],
            recv_sem=gate_recv.at[column, part],
            device_id=(target, mz),
            device_id_type=MESH,
        )

    pl.semaphore_wait(barrier, n - 1 + nz - 1)
    for cl in range(per_col):
        for k in range(1, n):
            target = device_at(lax.rem(place + n - k, n), n)
            gate_copy(cl, 2, target).start()

            for part in range(2):
                @pl.when(direct(me * per_col + cl, target, part))
                def _():
                    gate_copy(cl, part, target).start()
    for cl in range(per_col):
        column = me * per_col + cl
        phases[column] = stage_phase[cl]
        for part in range(2):
            gates[column, part] = stage[cl, part, pl.ds(place * own, own)]

    def pass_copy(column, part):
        return pltpu.make_async_remote_copy(
            src_ref=gates.at[column, part],
            dst_ref=gates.at[column, part],
            send_sem=pass_send.at[column, part],
            recv_sem=gate_recv.at[column, part],
            device_id=(me, partner),
            device_id_type=MESH,
        )

    def pass_on(column):
        for part in range(2):
            @pl.when(passes(column, part))
            def _():
                pass_copy(column, part).wait_recv()
                pass_copy(column, part).start()

    def wait_gates(column, part):
        sink = phases.at[column] if part == 2 else gates.at[column, part]
        needed = column // per_col != me
        if part < 2:
            needed = jnp.logical_and(needed, jnp.logical_not(passes(column, part)))

        @pl.when(needed)
        def _():
            pltpu.make_async_remote_copy(
                src_ref=sink,
                dst_ref=sink,
                send_sem=gate_send.at[0, part, 0],
                recv_sem=gate_recv.at[column, part],
                device_id=(lax.rem(me + 1, n), mz),
                device_id_type=MESH,
            ).wait_recv()

    def halo_copy(column, piece):
        part = pl.ds(piece * part_size, part_size)
        return pltpu.make_async_remote_copy(
            src_ref=board.at[column, 0, part],
            dst_ref=halo.at[column, part],
            send_sem=halo_send.at[column, piece],
            recv_sem=halo_recv.at[column, piece],
            device_id=(device_at(lax.rem(place + n - 1, n), n), mz),
            device_id_type=MESH,
        )

    def one_row(column, r, mixed, right_wait, send):
        left = gates[column, 0, r].astype(jnp.bfloat16)
        left = jnp.concatenate([left, left], axis=1)
        stacks = []
        for m in mixed:
            high, low = split(m)
            turned_high, turned_low = split(swap(m, width) * sign)
            stacks.append(jnp.concatenate([high, turned_high, low, turned_low], axis=0))
        middle = jnp.dot(
            left, jnp.concatenate(stacks, axis=1), preferred_element_type=jnp.float32
        )
        if right_wait:
            wait_gates(column, 1)
            wait_gates(column, 2)
        right = gates[column, 1, r]
        right = jnp.concatenate([right, swap(right, width) * sign], axis=0).astype(jnp.bfloat16)
        right = jnp.concatenate([right, right], axis=0)
        high, low = split(
            jnp.concatenate([middle[:, i * lanes:(i + 1) * lanes] for i in range(len(mixed))], axis=0)
        )
        outs = jnp.dot(
            jnp.concatenate([high, low], axis=1), right, preferred_element_type=jnp.float32
        )
        for s in range(slices):
            i = s if len(mixed) > 1 else 0
            out = outs[i * width:(i + 1) * width]
            if len(mixed) == 1 and s > 0:
                out_swapped = first_swapped
            else:
                out_swapped = swap(out, width)
                first_swapped = out_swapped
            turned = out * phases[column, pl.ds(s, 1), :] + out_swapped * phases[
                column, pl.ds(slices + s, 1), :
            ]
            board[column, r, s] = turned
            size = jnp.abs(turned).reshape(width // 8, 8, lanes)
            peak[s] = jnp.maximum(peak[s], jnp.max(size, axis=0))
            if send and (s + 1) % part_size == 0:
                @pl.when(place > 0)
                def _():
                    halo_copy(column, s // part_size).start()

    for load in loads[2:]:
        load.wait()
    for column in range(min(2, columns)):
        pass_on(column)
    wait_gates(0, 0)
    for r in range(own):
        below = edge_ref[r + 1].astype(jnp.float32)
        weight = 0.5 if r + 1 < own else jnp.where(last, 0.0, 0.5).astype(jnp.float32)
        mixed = edge_ref[r].astype(jnp.float32) + weight * below
        one_row(0, r, [mixed], r == 0, r == 0 and columns > 1)
        if r == 0 and columns > 2:
            pass_on(2)

    def column_step(column, scale, send):
        for part in range(3):
            wait_gates(column, part)
        for r in range(own):
            mixed = []
            for s in range(slices):
                if r + 1 == own and s % part_size == 0:
                    @pl.when(jnp.logical_not(last))
                    def _():
                        halo_copy(column - 1, s // part_size).wait_recv()
                below = board[column - 1, r + 1, s] if r + 1 < own else halo[column - 1, s]
                m = board[column - 1, r, s] + 0.5 * below
                mixed.append(m if scale is None else m * scale[s])
            one_row(column, r, mixed, False, send and r == 0)
            if r == 0:
                @pl.when(column + 2 < columns)
                def _():
                    pass_on(jnp.minimum(column + 2, columns - 1))

    def exchange(slot, count, index, axis_copy, sender, receiver):
        def copy(target):
            return axis_copy(slot, target)

        receiver[slot, index] = sender[slot]
        for k in range(1, count):
            copy(lax.rem(index + k, count)).start()
        for k in range(1, count):
            copy(lax.rem(index + k, count)).wait_send()

    def x_copy(slot, target):
        return pltpu.make_async_remote_copy(
            src_ref=xsend.at[slot],
            dst_ref=xrecv.at[slot, me],
            send_sem=x_send.at[slot, target],
            recv_sem=x_recv.at[slot, me],
            device_id=(target, mz),
            device_id_type=MESH,
        )

    def x_wait(slot):
        for k in range(1, n):
            source = lax.rem(me + k, n)
            pltpu.make_async_remote_copy(
                src_ref=xsend.at[slot],
                dst_ref=xrecv.at[slot, source],
                send_sem=x_send.at[slot, source],
                recv_sem=x_recv.at[slot, source],
                device_id=(source, mz),
                device_id_type=MESH,
            ).wait_recv()

    def z_copy(target):
        return pltpu.make_async_remote_copy(
            src_ref=zsend,
            dst_ref=zrecv.at[mz],
            send_sem=z_send.at[target],
            recv_sem=z_recv.at[mz],
            device_id=(me, target),
            device_id_type=MESH,
        )

    def local_peaks():
        return [
            jnp.max(jnp.max(peak[s], axis=0, keepdims=True), axis=1, keepdims=True)
            for s in range(slices)
        ]

    logs = [jnp.zeros((1, 1), jnp.float32)] * slices
    scale = None
    begin, slot = 1, 0
    while True:
        stop = min(columns, (begin // SEGMENT + 1) * SEGMENT)
        if scale is not None:
            column_step(begin, scale, begin + 1 < columns)
            begin += 1
        full = min(stop, columns - 1)

        def loop_step(column, carry):
            column_step(column, None, True)
            return carry

        if full > begin:
            lax.fori_loop(begin, full, loop_step, 0)
        if stop == columns:
            if columns - 1 >= begin:
                column_step(columns - 1, None, False)
            break
        for s, m in enumerate(local_peaks()):
            xsend[slot, pl.ds(s, 1), :] = jnp.broadcast_to(m, (1, lanes))
        exchange(slot, n, me, x_copy, xsend, xrecv)
        x_wait(slot)
        scale = []
        for s in range(slices):
            m = xrecv[slot, 0, pl.ds(s, 1), :]
            for d in range(1, n):
                m = jnp.maximum(m, xrecv[slot, d, pl.ds(s, 1), :])
            logs[s] = logs[s] + jnp.log(m[:, :1])
            scale.append(1.0 / m)
            peak[s] = jnp.ones(peak.shape[1:], jnp.float32)
        begin, slot = stop, slot + 1

    factor = 1.0 / math.sqrt(rows * width * width)
    mine = local_peaks()
    for s in range(slices):
        real = jnp.zeros((8, lanes), jnp.float32)
        imag = jnp.zeros((8, lanes), jnp.float32)
        inverse = 1.0 / mine[s]
        for r in range(own):
            close = close_ref[r]
            value = board[columns - 1, r, s] * inverse
            real = real + jnp.sum((value * close).reshape(width // 8, 8, lanes), axis=0)
            imag = imag + jnp.sum((value * swap(close, width)).reshape(width // 8, 8, lanes), axis=0)
        xsend[slot, pl.ds(s, 1), :] = jnp.sum(real, axis=0, keepdims=True) * (-sign)
        xsend[slot, pl.ds(slices + s, 1), :] = jnp.sum(imag, axis=0, keepdims=True)
        xsend[slot, pl.ds(2 * slices + s, 1), :] = jnp.broadcast_to(mine[s], (1, lanes))
    exchange(slot, n, me, x_copy, xsend, xrecv)
    x_wait(slot)
    all_peaks = [xrecv[slot, d, pl.ds(2 * slices, slices), :] for d in range(n)]
    top_peak = functools.reduce(jnp.maximum, all_peaks)
    inverse = 1.0 / top_peak
    real = jnp.zeros((slices, lanes), jnp.float32)
    imag = jnp.zeros((slices, lanes), jnp.float32)
    for d in range(n):
        ratio = all_peaks[d] * inverse
        real = real + xrecv[slot, d, pl.ds(0, slices), :] * ratio
        imag = imag + xrecv[slot, d, pl.ds(slices, slices), :] * ratio
    real = jnp.sum(real, axis=1, keepdims=True) * factor
    imag = jnp.sum(imag, axis=1, keepdims=True) * factor
    log = jnp.log(top_peak)[:, :1] + jnp.concatenate(logs, axis=0)
    result_ref[pl.ds(0, slices), :] = jnp.where(lane == 0, real, jnp.where(lane == 1, imag, log))
    top = jnp.max(log, axis=0, keepdims=True)
    share = jnp.exp(log - top)
    zsend[pl.ds(0, 1), :] = jnp.broadcast_to(jnp.sum(real * share, axis=0, keepdims=True), (1, lanes))
    zsend[pl.ds(1, 1), :] = jnp.broadcast_to(jnp.sum(imag * share, axis=0, keepdims=True), (1, lanes))
    zsend[pl.ds(2, 1), :] = jnp.broadcast_to(top, (1, lanes))
    zrecv[mz] = zsend[...]
    for k in range(1, nz):
        z_copy(lax.rem(mz + k, nz)).start()
    for k in range(1, nz):
        source = lax.rem(mz + k, nz)
        pltpu.make_async_remote_copy(
            src_ref=zsend,
            dst_ref=zrecv.at[source],
            send_sem=z_send.at[source],
            recv_sem=z_recv.at[source],
            device_id=(me, source),
            device_id_type=MESH,
        ).wait_recv()
    tops = [zrecv[z, pl.ds(2, 1), :] for z in range(nz)]
    top = functools.reduce(jnp.maximum, tops)
    real = jnp.zeros((1, lanes), jnp.float32)
    imag = jnp.zeros((1, lanes), jnp.float32)
    for z in range(nz):
        share = jnp.exp(tops[z] - top)
        real = real + zrecv[z, pl.ds(0, 1), :] * share
        imag = imag + zrecv[z, pl.ds(1, 1), :] * share
    result_ref[pl.ds(slices, 1), :] = jnp.where(lane == 0, real, jnp.where(lane == 1, imag, top))

    for k in range(1, nz):
        z_copy(lax.rem(mz + k, nz)).wait_send()
    for cl in range(per_col):
        for k in range(1, n):
            target = lax.rem(me + k, n)
            gate_copy(cl, 2, target).wait_send()

            for part in range(2):
                @pl.when(direct(me * per_col + cl, target, part))
                def _():
                    gate_copy(cl, part, target).wait_send()
    for column in range(columns):
        for part in range(2):
            @pl.when(passes(column, part))
            def _():
                pass_copy(column, part).wait_send()
    if columns > 1:
        @pl.when(place > 0)
        def _():
            for column in range(columns - 1):
                for piece in range(pieces):
                    halo_copy(column, piece).wait_send()


def unpack(result_ref, amp_ref, log_ref, total_ref, top_ref):
    slices = amp_ref.shape[1]
    for s in range(slices):
        for k in range(2):
            amp_ref[pl.ds(k, 1), pl.ds(s, 1)] = result_ref[pl.ds(s, 1), pl.ds(k, 1)]
        log_ref[:, pl.ds(s, 1)] = result_ref[pl.ds(s, 1), pl.ds(2, 1)]
    total_ref[...] = result_ref[pl.ds(slices, 1), pl.ds(0, 2)]
    top_ref[...] = result_ref[pl.ds(slices, 1), pl.ds(2, 1)]


def body(layout, assign, edge, gate_left, gate_right, phase_angle, close):
    n, nz = lax.axis_size("col"), lax.axis_size("cuts")
    rows, width, lanes = edge.shape
    per_col = gate_left.shape[0]
    columns, own, slices = n * per_col, rows // n, assign.shape[0]
    rounds = -(-columns // SEGMENT)
    pieces = 2 if slices % 2 == 0 else 1
    f32 = jnp.float32
    vmem = pl.BlockSpec(memory_space=pltpu.VMEM)
    hbm = pl.BlockSpec(memory_space=pltpu.HBM)
    smem = pl.BlockSpec(memory_space=pltpu.SMEM)
    dma = pltpu.SemaphoreType.DMA
    message = -(-3 * slices // 8) * 8
    phase_rows = -(-2 * slices // 8) * 8
    result = pl.pallas_call(
        functools.partial(kernel, n, nz, rows),
        out_shape=jax.ShapeDtypeStruct((-(-(slices + 1) // 8) * 8, lanes), f32),
        in_specs=[smem, smem, hbm, hbm, hbm, vmem, hbm],
        out_specs=vmem,
        scratch_shapes=[
            pltpu.VMEM((own + 1, width, lanes), edge.dtype),
            pltpu.VMEM(gate_left.shape, gate_left.dtype),
            pltpu.VMEM(gate_right.shape, gate_right.dtype),
            pltpu.VMEM((own, width, lanes), f32),
            pltpu.VMEM((phase_angle.shape[0], lanes), f32),
            pltpu.VMEM((phase_angle.shape[0], lanes), f32),
            dma((5,)),
            pltpu.VMEM((per_col, 2, rows, width, lanes), f32),
            pltpu.VMEM((per_col, phase_rows, lanes), f32),
            pltpu.VMEM((columns, 2, own, width, lanes), f32),
            pltpu.VMEM((columns, phase_rows, lanes), f32),
            pltpu.VMEM((columns, own, slices, width, lanes), f32),
            pltpu.VMEM((columns, slices, width, lanes), f32),
            pltpu.VMEM((slices, 8, lanes), f32),
            pltpu.VMEM((rounds, message, lanes), f32),
            pltpu.VMEM((rounds, n, message, lanes), f32),
            pltpu.VMEM((8, lanes), f32),
            pltpu.VMEM((nz, 8, lanes), f32),
            dma((per_col, 3, n)),
            dma((columns, 3)),
            dma((columns, 2)),
            dma((columns, pieces)),
            dma((columns, pieces)),
            dma((rounds, n)),
            dma((rounds, n)),
            dma((nz,)),
            dma((nz,)),
        ],
        compiler_params=pltpu.CompilerParams(
            collective_id=0, has_side_effects=True, vmem_limit_bytes=67_000_000
        ),
    )(layout.T, assign.T, edge, gate_left, gate_right, phase_angle, close)
    amp, log, total, top = pl.pallas_call(
        unpack,
        out_shape=[
            jax.ShapeDtypeStruct((2, slices), f32),
            jax.ShapeDtypeStruct((1, slices), f32),
            jax.ShapeDtypeStruct((1, 2), f32),
            jax.ShapeDtypeStruct((1, 1), f32),
        ],
        in_specs=[vmem],
        out_specs=[vmem] * 4,
    )(result)
    return amp.T, log.reshape(slices), total.reshape(2), top.reshape(())


def solution(mesh):
    in_specs = (
        P(None, "col"),
        P("cuts", "col"),
        P(),
        P("col", None, None, None),
        P("col", None, None, None),
        P(),
        P(),
    )
    out_specs = (P("cuts", None), P("cuts"), P(), P())
    return jax.shard_map(body, mesh=mesh, in_specs=in_specs, out_specs=out_specs, check_vma=False)
```
